256 devices in a mesh: ga: 64 (over y_hi, z, x), ta: 4 (over y_lo, core).
Axes of the slice: x: 4, y: 4 (y_hi: 2, y_lo: 2; y = y_hi * 2 + y_lo), z: 8, core: 2. Of those that a mesh axis runs over, the one named last changes fastest.
Arguments:
- density: bfloat16 [2, 6144, 16384], P(None, 'ga', 'ta'), may hold values from -6 to 6
- coulomb: float32 [6144], P('ga'), may hold values from 0.001275776 to 0.01275776
- row_block: int32 [1], replicated, may hold values from 0 to 67
Outputs:
- kernel: float32 [4, 4096, 2, 240], P('ta', 'ga')
The draws below stay inside these ranges and needn't reach their ends.
Inputs may be any that keep to these rules, and one draw needn't show every extreme that they name: The rows row_block * 240 to row_block * 240 + 239 lie among the 16384 transitions.
All inputs are finite; a program needn't handle non-finite values.
Results may differ from the reference program's by a relative error of at most 0.0025.
Values may be sent and summed in bfloat16 or wider, within the bound.
A program may use at most 64 MiB of HBM per device.

```python
import math
import jax
import jax.numpy as jnp
from jax import lax

NG = 6144
NC = 16384
RB = 240
N_TA = 4


def shard_levels(key, dims, shards, least, high):
    gain, own = 1.0, jax.random.fold_in(key, 6)
    for position, shards_of in shards:
        steps = jnp.exp(jax.random.uniform(jax.random.fold_in(own, position), (shards_of,), jnp.float32, least / len(shards), high / len(shards)))
        gain = gain * jnp.repeat(steps, dims[position] // shards_of).reshape([-1 if axis == position else 1 for axis in range(len(dims))])
    return gain


def gaussian(stream_key, shape, scale, most, split=(), held_as=jnp.bfloat16):
    drawn = jax.random.normal(stream_key, shape, jnp.float32) * scale
    if len(split) > 0:
        drawn = shard_levels(stream_key, shape, split, -0.22, 0.18) * drawn
    return jnp.clip(drawn, min=-most, max=most).astype(held_as)


def setup_inputs(seed: int = 0) -> dict:
    key_list = jax.random.split(jax.random.key(seed), 4)
    density = gaussian(key_list[0], (2, NG, NC), 1.0, 6.0, ((1, 64), (2, 4)))
    coulomb = jnp.clip(jnp.exp(math.log(0.01275776) - 2.3025851 * jax.random.uniform(key_list[1], (NG,), jnp.float32) ** shard_levels(key_list[1], (NG,), ((0, 64),), -0.2, 0.2)), 0.001275776, 0.01275776)
    row_block = jax.random.randint(key_list[2], (1,), 0, NC // RB).astype(jnp.int32)
    return dict(density=density, coulomb=coulomb, row_block=row_block)


def stack_left(folded):
    real_part = folded[0]
    imag_part = folded[1]
    upper_half = jnp.concatenate([real_part, -imag_part], axis=1)
    lower_half = jnp.concatenate([imag_part, real_part], axis=1)
    return jnp.concatenate([upper_half, lower_half], axis=0)


def reference(density, coulomb, row_block):
    offset = (row_block[0] * RB).astype(jnp.int32)
    picked = lax.dynamic_slice_in_dim(density, offset, RB, 2)
    folded = (coulomb[None, :, None] * picked.astype(jnp.float32)).astype(jnp.bfloat16)
    stacked = stack_left(folded)
    flattened = density.reshape(2 * NG, NC)
    kernel = lax.dot_general(flattened, stacked, (((0,), (0,)), ((), ())), preferred_element_type=jnp.float32)
    return kernel.reshape(N_TA, NC // N_TA, 2, RB)
```

```python
import jax
import jax.numpy as jnp
from jax import lax
from jax.experimental import pallas as pl
from jax.experimental.pallas import tpu as pltpu
from jax.sharding import PartitionSpec as P

MESH = pl.DeviceIdType.MESH
RB = 240
RBP = 256
G = 96
COLS = 4096
WIN = 384
NX, NY, NZ = 4, 2, 8
NA = NX * NY
ORDER = (2, 1, 3, 0)
NCH = len(ORDER)


def place(x, yh, z, yl, c):
    return (yh * (NZ * NX) + z * NX + x, yl * 2 + c)


def kernel(row_ref, coul_ref, dens_ref, out_ref, dv, wpart, s1buf, fbuf, fstack, sbuf, dbuf, zsend, zrecv, own,
           lsem, s1s, s1r, fs, fr, xs, xr, ds, dr, zs, zr):
    ga = lax.axis_index("ga")
    ta = lax.axis_index("ta")
    x, z, yh = ga % NX, (ga // NX) % NZ, ga // (NX * NZ)
    yl, c = ta // 2, ta % 2
    kz, par = z // 2, z % 2

    load = pltpu.make_async_copy(dens_ref, dv, lsem)
    load.start()

    def group(r):
        return place((x + r % NX) % NX, (yh + r // NX) % NY, z, yl, c)

    def along(delta, eps):
        return place(x, yh, 2 * ((kz + delta) % 4) + (par + eps) % 2, yl, c)

    def mates(q):
        return ((yl + q // 2) % 2, (c + q % 2) % 2)

    bar = pltpu.get_barrier_semaphore()
    for r in range(1, NA):
        pl.semaphore_signal(bar, inc=1, device_id=group(r), device_id_type=MESH)
    for s in range(1, NZ):
        pl.semaphore_signal(bar, inc=1, device_id=along(s // 2, s % 2), device_id_type=MESH)
    for q in range(1, 4):
        pl.semaphore_signal(bar, inc=1, device_id=place(x, yh, z, *mates(q)), device_id_type=MESH)

    load.wait()

    start = row_ref[0] * RB - ta * COLS
    tile = jnp.minimum(jnp.maximum(lax.shift_right_arithmetic(start, 7), 0), (COLS - WIN) // 128)
    src = lax.broadcasted_iota(jnp.int32, (WIN, RBP), 0) + tile * 128
    dst = lax.broadcasted_iota(jnp.int32, (WIN, RBP), 1)
    hit = jnp.logical_and(src == dst + start, dst < RB)
    onehot = jnp.where(hit, 1.0, 0.0).astype(jnp.bfloat16)
    weight = jnp.broadcast_to(coul_ref[...], (128, 128)).T[:G, :]
    weight = jnp.concatenate([weight, weight], axis=1)
    for part in range(2):
        window = dv[part, :, :WIN]
        for k in range(1, (COLS - WIN) // 128 + 1):
            window = jnp.where(tile == k, dv[part, :, k * 128:k * 128 + WIN], window)
        picked = jnp.dot(window, onehot, preferred_element_type=jnp.float32)
        wpart[part] = (weight * picked).astype(jnp.bfloat16)

    low = lax.broadcasted_iota(jnp.int32, (G, 128), 1) < 64

    def pack(j):
        zpair = 2 * ((kz + ORDER[j]) % 4)
        z0 = zpair + par
        z1 = zpair + (par + 1) % 2
        for part in range(2):
            for y in range(NY):
                for h in range(2):
                    o0 = pl.multiple_of((y * 16 + z0 * 2 + h) * 128, 128)
                    o1 = pl.multiple_of((y * 16 + z1 * 2 + h) * 128, 128)
                    t0 = dv[part, :, pl.ds(o0, 128)].astype(jnp.float32)
                    t1 = dv[part, :, pl.ds(o1, 128)].astype(jnp.float32)
                    even = jnp.where(low, t0, pltpu.roll(t1, 64, 1))
                    odd = jnp.where(low, pltpu.roll(t0, 64, 1), t1)
                    sbuf[j, y * NX + 2 * h, part * G:(part + 1) * G, :] = even.astype(jnp.bfloat16)
                    sbuf[j, y * NX + 2 * h + 1, part * G:(part + 1) * G, :] = odd.astype(jnp.bfloat16)
        dbuf[j, 0] = sbuf[j, yh * NX + x]

    waits = []

    def send(src, dst, ss, rs, device):
        cp = pltpu.make_async_remote_copy(src_ref=src, dst_ref=dst, send_sem=ss, recv_sem=rs, device_id=device,
                                          device_id_type=MESH)
        cp.start()
        waits.append(cp)
        return cp

    def spread(j):
        got = []
        for r in range(1, NA):
            dest = (yh + r // NX) % NY * NX + (x + r % NX) % NX
            got.append(send(sbuf.at[j, dest], dbuf.at[j, r], ds.at[j, r], dr.at[j, r], group(r)))
        return got

    pack(0)
    pl.semaphore_wait(bar, (NA - 1) + (NZ - 1) + 3)

    first = []
    for q in range(1, 4):
        ylq, cq = mates(q)
        first.append(send(wpart.at[cq], s1buf.at[q - 1], s1s.at[q - 1], s1r.at[q - 1], place(x, yh, z, ylq, cq)))
    arrived = [spread(0)]
    pack(1)
    for cp in first:
        cp.wait_recv()
    total = wpart[c].astype(jnp.float32)
    for q in range(3):
        total = total + s1buf[q].astype(jnp.float32)
    fbuf[0, c] = total.astype(jnp.bfloat16)
    rows = [send(fbuf.at[0, c], fbuf.at[r, c], fs.at[r], fr.at[r], group(r)) for r in range(1, NA)]
    other = place(x, yh, z, yl, (c + 1) % 2)
    across = [send(fbuf.at[0, c], fbuf.at[0, c], xs.at[0], xr.at[0], other)]
    arrived.append(spread(1))
    pack(2)
    arrived.append(spread(2))
    pack(3)
    arrived.append(spread(3))
    for r in range(1, NA):
        rows[r - 1].wait_recv()
        across.append(send(fbuf.at[r, c], fbuf.at[r, c], xs.at[r], xr.at[r], other))
    for r in range(NA):
        across[r].wait_recv()
        re = fbuf[r, 0]
        im = fbuf[r, 1]
        fstack[r * 2 * G:r * 2 * G + G, :RBP] = re
        fstack[r * 2 * G:r * 2 * G + G, RBP:] = -im
        fstack[r * 2 * G + G:(r + 1) * 2 * G, :RBP] = im
        fstack[r * 2 * G + G:(r + 1) * 2 * G, RBP:] = re

    sums = []
    for j in range(NCH):
        for cp in arrived[j]:
            cp.wait_recv()
        cols = dbuf[j].reshape(NA * 2 * G, 128)
        prod = lax.dot_general(cols, fstack[...], (((0,), (0,)), ((), ())), preferred_element_type=jnp.float32)
        for eps in range(2):
            slot = ORDER[j] * 2 + eps
            block = prod[eps * 64:(eps + 1) * 64]
            if slot == 0:
                own[...] = block
            else:
                zsend[slot] = block.astype(jnp.bfloat16)
                sums.append(send(zsend.at[slot], zrecv.at[slot], zs.at[slot], zr.at[slot], along(ORDER[j], eps)))
    acc = own[...]
    for cp, slot in zip(sums, [d * 2 + e for d in ORDER for e in range(2) if d * 2 + e > 0]):
        cp.wait_recv()
        acc = acc + zrecv[slot].astype(jnp.float32)
    out_ref[...] = acc
    for cp in waits:
        cp.wait_send()


def body(density, coulomb, row_block):
    weight = jnp.pad(coulomb.reshape(1, G), ((0, 0), (0, 128 - G)))
    dma = pltpu.SemaphoreType.DMA
    bf16, f32 = jnp.bfloat16, jnp.float32
    out = pl.pallas_call(
        kernel,
        out_shape=jax.ShapeDtypeStruct((64, 2 * RBP), f32),
        in_specs=[
            pl.BlockSpec(memory_space=pltpu.SMEM),
            pl.BlockSpec(memory_space=pltpu.VMEM),
            pl.BlockSpec(memory_space=pl.ANY),
        ],
        out_specs=pl.BlockSpec(memory_space=pltpu.VMEM),
        scratch_shapes=[
            pltpu.VMEM((2, G, COLS), bf16),
            pltpu.VMEM((2, G, RBP), bf16),
            pltpu.VMEM((3, G, RBP), bf16),
            pltpu.VMEM((NA, 2, G, RBP), bf16),
            pltpu.VMEM((NA * 2 * G, 2 * RBP), bf16),
            pltpu.VMEM((NCH, NA, 2 * G, 128), bf16),
            pltpu.VMEM((NCH, NA, 2 * G, 128), bf16),
            pltpu.VMEM((NZ, 64, 2 * RBP), bf16),
            pltpu.VMEM((NZ, 64, 2 * RBP), bf16),
            pltpu.VMEM((64, 2 * RBP), f32),
            dma, dma((3,)), dma((3,)), dma((NA,)), dma((NA,)), dma((NA,)), dma((NA,)),
            dma((NCH, NA)), dma((NCH, NA)), dma((NZ,)), dma((NZ,)),
        ],
        compiler_params=pltpu.CompilerParams(collective_id=0, has_side_effects=True),
        name="exchange",
    )(row_block, weight, density)
    return out.reshape(64, 2, RBP)[:, :, :RB].reshape(1, 64, 2, RB)


def solution(mesh):
    return jax.shard_map(
        body,
        mesh=mesh,
        in_specs=(P(None, "ga", "ta"), P("ga"), P()),
        out_specs=P("ta", "ga", None, None),
        check_vma=False,
    )
```

```python
import jax
import jax.numpy as jnp
from jax import lax
from jax.experimental import pallas as pl
from jax.experimental.pallas import tpu as pltpu
from jax.sharding import PartitionSpec as P

MESH = pl.DeviceIdType.MESH
RB = 240
RBP = 256
G = 96
COLS = 4096
WIN = 384
NX, NY, NZ = 4, 2, 8
ORDER = ((2, 1), (1, 1), (3, 1), (2, 0), (1, 0), (0, 1), (3, 0), (0, 0))
NP = len(ORDER)


def place(x, yh, z, yl, c):
    return (yh * (NZ * NX) + z * NX + x, yl * 2 + c)


def kernel(row_ref, coul_ref, dens_ref, out_ref, dv, wpart, s1buf, fbuf, fstack, sbuf, dbuf, ysend, yrecv, zsend, zrecv, own,
           lsem, s1s, s1r, fs, fr, xs, xr, ds, dr, ys, yr, zs, zr):
    ga = lax.axis_index("ga")
    ta = lax.axis_index("ta")
    x, z, yh = ga % NX, (ga // NX) % NZ, ga // (NX * NZ)
    yl, c = ta // 2, ta % 2
    kz, par = z // 2, z % 2
    other = (yh + 1) % 2

    load = pltpu.make_async_copy(dens_ref, dv, lsem)
    load.start()

    def beside(r):
        return place((x + r) % NX, yh, z, yl, c)

    def along(delta, eps):
        return place(x, yh, 2 * ((kz + delta) % 4) + (par + eps) % 2, yl, c)

    def mates(q):
        return ((yl + q // 2) % 2, (c + q % 2) % 2)

    opposite = place(x, other, z, yl, c)
    twin = place(x, yh, z, yl, (c + 1) % 2)

    bar = pltpu.get_barrier_semaphore()
    peers = [beside(r) for r in range(1, NX)] + [opposite] + [along(s // 2, s % 2) for s in range(1, NZ)]
    peers += [place(x, yh, z, *mates(q)) for q in range(1, 4)]
    for peer in peers:
        pl.semaphore_signal(bar, inc=1, device_id=peer, device_id_type=MESH)

    with jax.named_scope("load_wait"):
        load.wait()

    start = row_ref[0] * RB - ta * COLS
    tile = jnp.minimum(jnp.maximum(lax.shift_right_arithmetic(start, 7), 0), (COLS - WIN) // 128)
    src = lax.broadcasted_iota(jnp.int32, (WIN, RBP), 0) + tile * 128
    dst = lax.broadcasted_iota(jnp.int32, (WIN, RBP), 1)
    hit = jnp.logical_and(src == dst + start, dst < RB)
    onehot = jnp.where(hit, 1.0, 0.0).astype(jnp.bfloat16)
    diag = lax.broadcasted_iota(jnp.int32, (G, G), 0) == lax.broadcasted_iota(jnp.int32, (G, G), 1)
    weight = jnp.sum(jnp.where(diag, jnp.broadcast_to(coul_ref[...], (G, G)), 0.0), axis=1, keepdims=True)
    for part in range(2):
        window = dv[part, :, :WIN]
        for k in range(1, (COLS - WIN) // 128 + 1):
            window = jnp.where(tile == k, dv[part, :, k * 128:k * 128 + WIN], window)
        picked = jnp.dot(window, onehot, preferred_element_type=jnp.float32)
        wpart[part] = (weight * picked).astype(jnp.bfloat16)

    low = lax.broadcasted_iota(jnp.int32, (G, 128), 1) < 64

    def pack(p):
        delta, w = ORDER[p]
        y = (yh + w) % NY
        zpair = 2 * ((kz + delta) % 4)
        z0 = zpair + par
        z1 = zpair + (par + 1) % 2
        for part in range(2):
            for h in range(2):
                o0 = pl.multiple_of((y * 16 + z0 * 2 + h) * 128, 128)
                o1 = pl.multiple_of((y * 16 + z1 * 2 + h) * 128, 128)
                t0 = dv[part, :, pl.ds(o0, 128)].astype(jnp.float32)
                t1 = dv[part, :, pl.ds(o1, 128)].astype(jnp.float32)
                even = jnp.where(low, t0, pltpu.roll(t1, 64, 1))
                odd = jnp.where(low, pltpu.roll(t0, 64, 1), t1)
                sbuf[p, 2 * h, part * G:(part + 1) * G, :] = even.astype(jnp.bfloat16)
                sbuf[p, 2 * h + 1, part * G:(part + 1) * G, :] = odd.astype(jnp.bfloat16)
        dbuf[p, 0] = sbuf[p, x]

    waits = []

    def send(src, dst, ss, rs, device):
        cp = pltpu.make_async_remote_copy(src_ref=src, dst_ref=dst, send_sem=ss, recv_sem=rs, device_id=device,
                                          device_id_type=MESH)
        cp.start()
        waits.append(cp)
        return cp

    def spread(p):
        return [send(sbuf.at[p, (x + r) % NX], dbuf.at[p, r], ds.at[p, r], dr.at[p, r], beside(r)) for r in range(1, NX)]

    with jax.named_scope("pack0"):
        pack(0)
    with jax.named_scope("bar_wait"):
        pl.semaphore_wait(bar, len(peers))

    first = []
    for q in range(1, 4):
        ylq, cq = mates(q)
        first.append(send(wpart.at[cq], s1buf.at[q - 1], s1s.at[q - 1], s1r.at[q - 1], place(x, yh, z, ylq, cq)))
    arrived = [spread(0)]
    with jax.named_scope("pack1"):
        pack(1)
        pack(2)
    with jax.named_scope("s1_wait"):
        for cp in first:
            cp.wait_recv()
    total = wpart[c].astype(jnp.float32)
    for q in range(3):
        total = total + s1buf[q].astype(jnp.float32)
    fbuf[0, c] = total.astype(jnp.bfloat16)
    rows = [send(fbuf.at[0, c], fbuf.at[r, c], fs.at[r], fr.at[r], beside(r)) for r in range(1, NX)]
    across = [send(fbuf.at[0, c], fbuf.at[0, c], xs.at[0], xr.at[0], twin)]
    arrived.append(spread(1))
    arrived.append(spread(2))
    with jax.named_scope("packs"):
        for p in range(3, NP):
            pack(p)
            arrived.append(spread(p))
    for r in range(1, NX):
        with jax.named_scope(f"rows_wait{r}"):
            rows[r - 1].wait_recv()
        across.append(send(fbuf.at[r, c], fbuf.at[r, c], xs.at[r], xr.at[r], twin))
    for r in range(NX):
        with jax.named_scope(f"across_wait{r}"):
            across[r].wait_recv()
        re = fbuf[r, 0]
        im = fbuf[r, 1]
        fstack[r * 2 * G:r * 2 * G + G, :RBP] = re
        fstack[r * 2 * G:r * 2 * G + G, RBP:] = -im
        fstack[r * 2 * G + G:(r + 1) * 2 * G, :RBP] = im
        fstack[r * 2 * G + G:(r + 1) * 2 * G, RBP:] = re

    halves = {}
    sums = []
    for p, (delta, w) in enumerate(ORDER):
        with jax.named_scope(f"piece_wait{p}"):
            for cp in arrived[p]:
                cp.wait_recv()
        cols = dbuf[p].reshape(NX * 2 * G, 128)
        prod = lax.dot_general(cols, fstack[...], (((0,), (0,)), ((), ())), preferred_element_type=jnp.float32)
        if w:
            ysend[delta] = prod.astype(jnp.bfloat16)
            halves[delta] = send(ysend.at[delta], yrecv.at[delta], ys.at[delta], yr.at[delta], opposite)
        else:
            with jax.named_scope(f"half_wait{p}"):
                halves[delta].wait_recv()
            both = prod + yrecv[delta].astype(jnp.float32)
            for eps in range(2):
                slot = delta * 2 + eps
                block = both[eps * 64:(eps + 1) * 64]
                if slot == 0:
                    own[...] = block
                else:
                    zsend[slot] = block.astype(jnp.bfloat16)
                    cp = send(zsend.at[slot], zrecv.at[slot], zs.at[slot], zr.at[slot], along(delta, eps))
                    sums.append((cp, slot))
    acc = own[...]
    for cp, slot in sums:
        with jax.named_scope(f"zwait{slot}"):
            cp.wait_recv()
        acc = acc + zrecv[slot].astype(jnp.float32)
    out_ref[:, 0, :] = acc[:, :RB]
    out_ref[:, 1, :] = acc[:, RBP:RBP + RB]
    with jax.named_scope("send_waits"):
        for cp in waits:
            cp.wait_send()


def body(density, coulomb, row_block):
    dma = pltpu.SemaphoreType.DMA
    bf16, f32 = jnp.bfloat16, jnp.float32
    out = pl.pallas_call(
        kernel,
        out_shape=jax.ShapeDtypeStruct((64, 2, RB), f32),
        in_specs=[
            pl.BlockSpec(memory_space=pltpu.SMEM),
            pl.BlockSpec(memory_space=pltpu.VMEM),
            pl.BlockSpec(memory_space=pl.ANY),
        ],
        out_specs=pl.BlockSpec(memory_space=pltpu.VMEM),
        scratch_shapes=[
            pltpu.VMEM((2, G, COLS), bf16),
            pltpu.VMEM((2, G, RBP), bf16),
            pltpu.VMEM((3, G, RBP), bf16),
            pltpu.VMEM((NX, 2, G, RBP), bf16),
            pltpu.VMEM((NX * 2 * G, 2 * RBP), bf16),
            pltpu.VMEM((NP, NX, 2 * G, 128), bf16),
            pltpu.VMEM((NP, NX, 2 * G, 128), bf16),
            pltpu.VMEM((4, 128, 2 * RBP), bf16),
            pltpu.VMEM((4, 128, 2 * RBP), bf16),
            pltpu.VMEM((NZ, 64, 2 * RBP), bf16),
            pltpu.VMEM((NZ, 64, 2 * RBP), bf16),
            pltpu.VMEM((64, 2 * RBP), f32),
            dma, dma((3,)), dma((3,)), dma((NX,)), dma((NX,)), dma((NX,)), dma((NX,)),
            dma((NP, NX)), dma((NP, NX)), dma((4,)), dma((4,)), dma((NZ,)), dma((NZ,)),
        ],
        compiler_params=pltpu.CompilerParams(collective_id=0, has_side_effects=True),
        name="exchange",
    )(row_block, coulomb.reshape(1, G), density)
    return out.reshape(1, 64, 2, RB)


def solution(mesh):
    return jax.shard_map(
        body,
        mesh=mesh,
        in_specs=(P(None, "ga", "ta"), P("ga"), P()),
        out_specs=P("ta", "ga", None, None),
        check_vma=False,
    )
```

```python
import jax
import jax.numpy as jnp
from jax import lax
from jax.experimental import pallas as pl
from jax.experimental.pallas import tpu as pltpu
from jax.sharding import PartitionSpec as P

MESH = pl.DeviceIdType.MESH
RB = 240
RBP = 256
G = 96
COLS = 4096
WIN = 384
NX, NY, NZ = 4, 2, 8
ORDER = ((2, 1), (3, 1), (1, 1), (2, 0), (0, 1), (3, 0), (1, 0), (0, 0))
NP = len(ORDER)


def place(x, yh, z, yl, c):
    return (yh * (NZ * NX) + z * NX + x, yl * 2 + c)


def kernel(row_hbm, coul_hbm, dens_ref, out_ref, row_ref, coul_ref, dv, wpart, s1buf, fbuf, fstack, sbuf, dbuf, ysend, yrecv, zsend, zrecv, own,
           lsem, ready, s1s, s1r, fs, fr, xs, xr, ds, dr, ys, yr, zs, zr):
    ga = lax.axis_index("ga")
    ta = lax.axis_index("ta")
    x, z, yh = ga % NX, (ga // NX) % NZ, ga // (NX * NZ)
    yl, c = ta // 2, ta % 2
    kz, par = z // 2, z % 2
    other = (yh + 1) % 2

    loads = [pltpu.make_async_copy(a, b, lsem.at[i])
             for i, (a, b) in enumerate(((dens_ref, dv), (row_hbm, row_ref), (coul_hbm, coul_ref)))]
    for load in loads:
        load.start()

    def pair(m):
        a, b = kz // 2, kz % 2
        return (a + m // 2) % 2 * 2 + (b + m % 2) % 2

    def beside(r):
        return place((x + r) % NX, yh, z, yl, c)

    def along(delta, eps):
        return place(x, yh, 2 * pair(delta) + (par + eps) % 2, yl, c)

    def mates(q):
        return ((yl + q // 2) % 2, (c + q % 2) % 2)

    opposite = place(x, other, z, yl, c)
    twin = place(x, yh, z, yl, (c + 1) % 2)

    bar = pltpu.get_barrier_semaphore()
    peers = [beside(r) for r in range(1, NX)] + [opposite]
    peers += [place(x, yh, z, *mates(q)) for q in range(1, 4)]
    for peer in peers:
        pl.semaphore_signal(bar, inc=1, device_id=peer, device_id_type=MESH)

    def greet(sem, d):
        @pl.when(z + d < NZ)
        def _():
            pl.semaphore_signal(sem, inc=1, device_id=place(x, yh, z + d, yl, c), device_id_type=MESH)

        @pl.when(z >= d)
        def _():
            pl.semaphore_signal(sem, inc=1, device_id=place(x, yh, z - d, yl, c), device_id_type=MESH)

    def met(d):
        return jnp.where(z + d < NZ, 1, 0) + jnp.where(z >= d, 1, 0)

    greet(bar, 1)

    with jax.named_scope("load_wait"):
        for load in loads:
            load.wait()

    start = row_ref[0] * RB - ta * COLS
    tile = jnp.minimum(jnp.maximum(lax.shift_right_arithmetic(start, 7), 0), (COLS - WIN) // 128)
    src = lax.broadcasted_iota(jnp.int32, (WIN, RBP), 0) + tile * 128
    dst = lax.broadcasted_iota(jnp.int32, (WIN, RBP), 1)
    hit = jnp.logical_and(src == dst + start, dst < RB)
    onehot = jnp.where(hit, 1.0, 0.0).astype(jnp.bfloat16)
    diag = lax.broadcasted_iota(jnp.int32, (G, G), 0) == lax.broadcasted_iota(jnp.int32, (G, G), 1)
    weight = jnp.sum(jnp.where(diag, jnp.broadcast_to(coul_ref[...], (G, G)), 0.0), axis=1, keepdims=True)
    for part in range(2):
        window = dv[part, :, :WIN]
        for k in range(1, (COLS - WIN) // 128 + 1):
            window = jnp.where(tile == k, dv[part, :, k * 128:k * 128 + WIN], window)
        picked = jnp.dot(window, onehot, preferred_element_type=jnp.float32)
        wpart[part] = (weight * picked).astype(jnp.bfloat16)

    low = lax.broadcasted_iota(jnp.int32, (G, 128), 1) < 64

    def pack(p):
        delta, w = ORDER[p]
        y = (yh + w) % NY
        zpair = 2 * pair(delta)
        z0 = zpair + par
        z1 = zpair + (par + 1) % 2
        for part in range(2):
            for h in range(2):
                o0 = pl.multiple_of((y * 16 + z0 * 2 + h) * 128, 128)
                o1 = pl.multiple_of((y * 16 + z1 * 2 + h) * 128, 128)
                t0 = dv[part, :, pl.ds(o0, 128)].astype(jnp.float32)
                t1 = dv[part, :, pl.ds(o1, 128)].astype(jnp.float32)
                even = jnp.where(low, t0, pltpu.roll(t1, 64, 1))
                odd = jnp.where(low, pltpu.roll(t0, 64, 1), t1)
                sbuf[p, 2 * h, part * G:(part + 1) * G, :] = even.astype(jnp.bfloat16)
                sbuf[p, 2 * h + 1, part * G:(part + 1) * G, :] = odd.astype(jnp.bfloat16)
        dbuf[p, 0] = sbuf[p, x]

    waits = []

    def send(src, dst, ss, rs, device):
        cp = pltpu.make_async_remote_copy(src_ref=src, dst_ref=dst, send_sem=ss, recv_sem=rs, device_id=device,
                                          device_id_type=MESH)
        cp.start()
        waits.append(cp)
        return cp

    def spread(p):
        return [send(sbuf.at[p, (x + r) % NX], dbuf.at[p, r], ds.at[p, r], dr.at[p, r], beside(r)) for r in range(1, NX)]

    with jax.named_scope("pack0"):
        pack(0)
    with jax.named_scope("bar_wait"):
        pl.semaphore_wait(bar, len(peers) + met(1))

    first = []
    for q in range(1, 4):
        ylq, cq = mates(q)
        first.append(send(wpart.at[cq], s1buf.at[q - 1], s1s.at[q - 1], s1r.at[q - 1], place(x, yh, z, ylq, cq)))
    arrived = [spread(0)]
    greet(ready.at[0], 1)
    with jax.named_scope("packs"):
        for p in range(1, NP):
            pack(p)
    with jax.named_scope("ready0"):
        pl.semaphore_wait(ready.at[0], met(1))
    greet(ready.at[1], 2)
    with jax.named_scope("s1_wait"):
        for cp in first:
            cp.wait_recv()
    total = wpart[c].astype(jnp.float32)
    for q in range(3):
        total = total + s1buf[q].astype(jnp.float32)
    fbuf[0, c] = total.astype(jnp.bfloat16)
    rows = [send(fbuf.at[0, c], fbuf.at[r, c], fs.at[r], fr.at[r], beside(r)) for r in range(1, NX)]
    del waits[-len(rows):]
    across = [send(fbuf.at[0, c], fbuf.at[0, c], xs.at[0], xr.at[0], twin)]
    with jax.named_scope("rows_sent"):
        for cp in rows:
            cp.wait_send()
    for p in range(1, NP):
        arrived.append(spread(p))
    with jax.named_scope("ready1"):
        pl.semaphore_wait(ready.at[1], met(2))
    greet(ready.at[2], 4)
    for r in range(1, NX):
        with jax.named_scope(f"rows_wait{r}"):
            rows[r - 1].wait_recv()
        across.append(send(fbuf.at[r, c], fbuf.at[r, c], xs.at[r], xr.at[r], twin))
    for r in range(NX):
        with jax.named_scope(f"across_wait{r}"):
            across[r].wait_recv()
        re = fbuf[r, 0]
        im = fbuf[r, 1]
        fstack[r * 2 * G:r * 2 * G + G, :RBP] = re
        fstack[r * 2 * G:r * 2 * G + G, RBP:] = -im
        fstack[r * 2 * G + G:(r + 1) * 2 * G, :RBP] = im
        fstack[r * 2 * G + G:(r + 1) * 2 * G, RBP:] = re

    halves = {}
    sums = []
    greeted = False
    for p, (delta, w) in enumerate(ORDER):
        with jax.named_scope(f"piece_wait{p}"):
            for cp in arrived[p]:
                cp.wait_recv()
        cols = dbuf[p].reshape(NX * 2 * G, 128)
        prod = lax.dot_general(cols, fstack[...], (((0,), (0,)), ((), ())), preferred_element_type=jnp.float32)
        if w:
            ysend[delta] = prod.astype(jnp.bfloat16)
            halves[delta] = send(ysend.at[delta], yrecv.at[delta], ys.at[delta], yr.at[delta], opposite)
        else:
            with jax.named_scope(f"half_wait{p}"):
                halves[delta].wait_recv()
            if not greeted:
                greeted = True
                with jax.named_scope("ready2"):
                    pl.semaphore_wait(ready.at[2], met(4))
            both = prod + yrecv[delta].astype(jnp.float32)
            for eps in range(2):
                slot = delta * 2 + eps
                block = both[eps * 64:(eps + 1) * 64]
                if slot == 0:
                    own[...] = block
                else:
                    zsend[slot] = block.astype(jnp.bfloat16)
                    cp = send(zsend.at[slot], zrecv.at[slot], zs.at[slot], zr.at[slot], along(delta, eps))
                    sums.append((cp, slot))
    acc = own[...]
    for cp, slot in sums:
        with jax.named_scope(f"zwait{slot}"):
            cp.wait_recv()
        acc = acc + zrecv[slot].astype(jnp.float32)
    out_ref[:, 0, :] = acc[:, :RB]
    out_ref[:, 1, :] = acc[:, RBP:RBP + RB]
    with jax.named_scope("send_waits"):
        for cp in waits:
            cp.wait_send()


def body(density, coulomb, row_block):
    dma = pltpu.SemaphoreType.DMA
    bf16, f32 = jnp.bfloat16, jnp.float32
    out = pl.pallas_call(
        kernel,
        out_shape=pltpu.VMEM((64, 2, RB), f32),
        in_specs=[pl.BlockSpec(memory_space=pltpu.HBM)] * 3,
        out_specs=pl.BlockSpec(memory_space=pltpu.VMEM),
        scratch_shapes=[
            pltpu.SMEM((1,), jnp.int32),
            pltpu.VMEM((1, G), f32),
            pltpu.VMEM((2, G, COLS), bf16),
            pltpu.VMEM((2, G, RBP), bf16),
            pltpu.VMEM((3, G, RBP), bf16),
            pltpu.VMEM((NX, 2, G, RBP), bf16),
            pltpu.VMEM((NX * 2 * G, 2 * RBP), bf16),
            pltpu.VMEM((NP, NX, 2 * G, 128), bf16),
            pltpu.VMEM((NP, NX, 2 * G, 128), bf16),
            pltpu.VMEM((4, 128, 2 * RBP), bf16),
            pltpu.VMEM((4, 128, 2 * RBP), bf16),
            pltpu.VMEM((NZ, 64, 2 * RBP), bf16),
            pltpu.VMEM((NZ, 64, 2 * RBP), bf16),
            pltpu.VMEM((64, 2 * RBP), f32),
            dma((3,)), pltpu.SemaphoreType.REGULAR((3,)), dma((3,)), dma((3,)), dma((NX,)), dma((NX,)), dma((NX,)), dma((NX,)),
            dma((NP, NX)), dma((NP, NX)), dma((4,)), dma((4,)), dma((NZ,)), dma((NZ,)),
        ],
        compiler_params=pltpu.CompilerParams(collective_id=0, has_side_effects=True),
        name="exchange",
    )(row_block, coulomb.reshape(1, G), density)
    return out.reshape(1, 64, 2, RB)


def solution(mesh):
    return jax.shard_map(
        body,
        mesh=mesh,
        in_specs=(P(None, "ga", "ta"), P("ga"), P()),
        out_specs=P("ta", "ga", None, None),
        check_vma=False,
    )
```

```python
import jax
import jax.numpy as jnp
from jax import lax
from jax.experimental import pallas as pl
from jax.experimental.pallas import tpu as pltpu
from jax.sharding import PartitionSpec as P

MESH = pl.DeviceIdType.MESH
RB = 240
RBP = 256
G = 96
COLS = 4096
WIN = 384
NX, NY, NZ = 4, 2, 8
Q = 48
ORDER = ((2, 1), (3, 1), (2, 0), (1, 1), (3, 0), (0, 1), (1, 0), (0, 0))
NP = len(ORDER)


def place(x, yh, z, yl, c):
    return (yh * (NZ * NX) + z * NX + x, yl * 2 + c)


def kernel(row_hbm, coul_hbm, dens_ref, out_ref, row_ref, coul_ref, dv, wpart, s1buf, fbuf, fstack, sbuf, dbuf, ysend, yrecv, zsend, zrecv, own,
           lsem, ready, s1s, s1r, fs, fr, xs, xr, ds, dr, ys, yr, zs, zr):
    ga = lax.axis_index("ga")
    ta = lax.axis_index("ta")
    x, z, yh = ga % NX, (ga // NX) % NZ, ga // (NX * NZ)
    yl, c = ta // 2, ta % 2
    kz, par = z // 2, z % 2
    other = (yh + 1) % 2

    loads = [pltpu.make_async_copy(a, b, lsem.at[i])
             for i, (a, b) in enumerate(((dens_ref, dv), (row_hbm, row_ref), (coul_hbm, coul_ref)))]
    for load in loads:
        load.start()

    def pair(m):
        a, b = kz // 2, kz % 2
        return (a + m // 2) % 2 * 2 + (b + m % 2) % 2

    def beside(r):
        return place((x + r) % NX, yh, z, yl, c)

    def along(delta, eps):
        return place(x, yh, 2 * pair(delta) + (par + eps) % 2, yl, c)

    def mates(q):
        return ((yl + q // 2) % 2, (c + q % 2) % 2)

    opposite = place(x, other, z, yl, c)
    twin = place(x, yh, z, yl, (c + 1) % 2)

    bar = pltpu.get_barrier_semaphore()
    peers = [opposite] + [place(x, yh, z, *mates(q)) for q in range(1, 4)]
    peers += [place((x + r) % NX, yh, z, (yl + u) % 2, c) for r in range(1, NX) for u in range(2)]
    for peer in peers:
        pl.semaphore_signal(bar, inc=1, device_id=peer, device_id_type=MESH)

    def greet(sem, d):
        @pl.when(z + d < NZ)
        def _():
            pl.semaphore_signal(sem, inc=1, device_id=place(x, yh, z + d, yl, c), device_id_type=MESH)

        @pl.when(z >= d)
        def _():
            pl.semaphore_signal(sem, inc=1, device_id=place(x, yh, z - d, yl, c), device_id_type=MESH)

    def met(d):
        return jnp.where(z + d < NZ, 1, 0) + jnp.where(z >= d, 1, 0)

    greet(bar, 1)

    with jax.named_scope("load_wait"):
        for load in loads:
            load.wait()

    start = row_ref[0] * RB - ta * COLS
    tile = jnp.minimum(jnp.maximum(lax.shift_right_arithmetic(start, 7), 0), (COLS - WIN) // 128)
    src = lax.broadcasted_iota(jnp.int32, (WIN, RBP), 0) + tile * 128
    dst = lax.broadcasted_iota(jnp.int32, (WIN, RBP), 1)
    hit = jnp.logical_and(src == dst + start, dst < RB)
    onehot = jnp.where(hit, 1.0, 0.0).astype(jnp.bfloat16)
    diag = lax.broadcasted_iota(jnp.int32, (G, G), 0) == lax.broadcasted_iota(jnp.int32, (G, G), 1)
    weight = jnp.sum(jnp.where(diag, jnp.broadcast_to(coul_ref[...], (G, G)), 0.0), axis=1, keepdims=True)
    for part in range(2):
        window = dv[part, :, :WIN]
        for k in range(1, (COLS - WIN) // 128 + 1):
            window = jnp.where(tile == k, dv[part, :, k * 128:k * 128 + WIN], window)
        picked = jnp.dot(window, onehot, preferred_element_type=jnp.float32)
        weighted = (weight * picked).astype(jnp.bfloat16)
        wpart[2 * part] = weighted[:Q]
        wpart[2 * part + 1] = weighted[Q:]

    low = lax.broadcasted_iota(jnp.int32, (G, 128), 1) < 64

    def pack(p):
        delta, w = ORDER[p]
        y = (yh + w) % NY
        zpair = 2 * pair(delta)
        z0 = zpair + par
        z1 = zpair + (par + 1) % 2
        for part in range(2):
            for h in range(2):
                o0 = pl.multiple_of((y * 16 + z0 * 2 + h) * 128, 128)
                o1 = pl.multiple_of((y * 16 + z1 * 2 + h) * 128, 128)
                t0 = dv[part, :, pl.ds(o0, 128)].astype(jnp.float32)
                t1 = dv[part, :, pl.ds(o1, 128)].astype(jnp.float32)
                even = jnp.where(low, t0, pltpu.roll(t1, 64, 1))
                odd = jnp.where(low, pltpu.roll(t0, 64, 1), t1)
                sbuf[p, 2 * h, part * G:(part + 1) * G, :] = even.astype(jnp.bfloat16)
                sbuf[p, 2 * h + 1, part * G:(part + 1) * G, :] = odd.astype(jnp.bfloat16)
        dbuf[p, 0] = sbuf[p, x]

    waits = []

    def send(src, dst, ss, rs, device):
        cp = pltpu.make_async_remote_copy(src_ref=src, dst_ref=dst, send_sem=ss, recv_sem=rs, device_id=device,
                                          device_id_type=MESH)
        cp.start()
        waits.append(cp)
        return cp

    def spread(p):
        return [send(sbuf.at[p, (x + r) % NX], dbuf.at[p, r], ds.at[p, r], dr.at[p, r], beside(r)) for r in range(1, NX)]

    with jax.named_scope("pack0"):
        pack(0)
    with jax.named_scope("bar_wait"):
        pl.semaphore_wait(bar, len(peers) + met(1))

    first = []
    for q in range(1, 4):
        ylq, cq = mates(q)
        first.append(send(wpart.at[ylq * 2 + cq], s1buf.at[q - 1], s1s.at[q - 1], s1r.at[q - 1], place(x, yh, z, ylq, cq)))
    arrived = [spread(0)]
    greet(ready.at[0], 1)
    with jax.named_scope("packs"):
        for p in range(1, NP):
            pack(p)
    with jax.named_scope("ready0"):
        pl.semaphore_wait(ready.at[0], met(1))
    greet(ready.at[1], 2)
    with jax.named_scope("s1_wait"):
        for cp in first:
            cp.wait_recv()
    total = wpart[ta].astype(jnp.float32)
    for q in range(3):
        total = total + s1buf[q].astype(jnp.float32)
    fbuf[0, ta] = total.astype(jnp.bfloat16)
    rows, across = [None], []
    for n in range(1, 2 * NX):
        r, u = n // 2, n % 2
        dest = place((x + r) % NX, yh, z, (yl + u) % 2, c)
        rows.append(send(fbuf.at[0, ta], fbuf.at[r, ta], fs.at[n], fr.at[n], dest))
    across.append(send(fbuf.at[0, ta], fbuf.at[0, ta], xs.at[0], xr.at[0], twin))
    for p in range(1, NP):
        arrived.append(spread(p))
    with jax.named_scope("ready1"):
        pl.semaphore_wait(ready.at[1], met(2))
    greet(ready.at[2], 4)
    for n in range(1, 2 * NX):
        r, u = n // 2, n % 2
        with jax.named_scope(f"rows_wait{n}"):
            rows[n].wait_recv()
        part = fbuf.at[r, (yl + u) % 2 * 2 + c]
        across.append(send(part, part, xs.at[n], xr.at[n], twin))
    for r in range(NX):
        with jax.named_scope(f"across_wait{r}"):
            across[2 * r].wait_recv()
            across[2 * r + 1].wait_recv()
        re = fbuf[r, 0:2].reshape(G, RBP)
        im = fbuf[r, 2:4].reshape(G, RBP)
        fstack[r * 2 * G:r * 2 * G + G, :RBP] = re
        fstack[r * 2 * G:r * 2 * G + G, RBP:] = -im
        fstack[r * 2 * G + G:(r + 1) * 2 * G, :RBP] = im
        fstack[r * 2 * G + G:(r + 1) * 2 * G, RBP:] = re

    halves = {}
    sums = []
    greeted = False
    for p, (delta, w) in enumerate(ORDER):
        with jax.named_scope(f"piece_wait{p}"):
            for cp in arrived[p]:
                cp.wait_recv()
        cols = dbuf[p].reshape(NX * 2 * G, 128)
        prod = lax.dot_general(cols, fstack[...], (((0,), (0,)), ((), ())), preferred_element_type=jnp.float32)
        if w:
            ysend[delta] = prod.astype(jnp.bfloat16)
            for eps in range(2):
                part = pl.ds(eps * 64, 64)
                halves[delta, eps] = send(ysend.at[delta, part], yrecv.at[delta, part], ys.at[2 * delta + eps],
                                          yr.at[2 * delta + eps], opposite)
        else:
            if not greeted:
                greeted = True
                with jax.named_scope("ready2"):
                    pl.semaphore_wait(ready.at[2], met(4))
            for eps in range(2):
                slot = delta * 2 + eps
                with jax.named_scope(f"half_wait{p}{eps}"):
                    halves[delta, eps].wait_recv()
                part = slice(eps * 64, (eps + 1) * 64)
                block = prod[part] + yrecv[delta, part].astype(jnp.float32)
                if slot == 0:
                    own[...] = block
                else:
                    zsend[slot] = block.astype(jnp.bfloat16)
                    cp = send(zsend.at[slot], zrecv.at[slot], zs.at[slot], zr.at[slot], along(delta, eps))
                    sums.append((cp, slot))
    acc = own[...]
    for cp, slot in sums:
        with jax.named_scope(f"zwait{slot}"):
            cp.wait_recv()
        acc = acc + zrecv[slot].astype(jnp.float32)
    out_ref[:, 0, :] = acc[:, :RB]
    out_ref[:, 1, :] = acc[:, RBP:RBP + RB]
    with jax.named_scope("send_waits"):
        for cp in waits:
            cp.wait_send()


def body(density, coulomb, row_block):
    dma = pltpu.SemaphoreType.DMA
    bf16, f32 = jnp.bfloat16, jnp.float32
    out = pl.pallas_call(
        kernel,
        out_shape=pltpu.VMEM((64, 2, RB), f32),
        in_specs=[pl.BlockSpec(memory_space=pltpu.HBM)] * 3,
        out_specs=pl.BlockSpec(memory_space=pltpu.VMEM),
        scratch_shapes=[
            pltpu.SMEM((1,), jnp.int32),
            pltpu.VMEM((1, G), f32),
            pltpu.VMEM((2, G, COLS), bf16),
            pltpu.VMEM((4, Q, RBP), bf16),
            pltpu.VMEM((3, Q, RBP), bf16),
            pltpu.VMEM((NX, 4, Q, RBP), bf16),
            pltpu.VMEM((NX * 2 * G, 2 * RBP), bf16),
            pltpu.VMEM((NP, NX, 2 * G, 128), bf16),
            pltpu.VMEM((NP, NX, 2 * G, 128), bf16),
            pltpu.VMEM((4, 128, 2 * RBP), bf16),
            pltpu.VMEM((4, 128, 2 * RBP), bf16),
            pltpu.VMEM((NZ, 64, 2 * RBP), bf16),
            pltpu.VMEM((NZ, 64, 2 * RBP), bf16),
            pltpu.VMEM((64, 2 * RBP), f32),
            dma((3,)), pltpu.SemaphoreType.REGULAR((3,)), dma((3,)), dma((3,)), dma((2 * NX,)), dma((2 * NX,)), dma((2 * NX,)), dma((2 * NX,)),
            dma((NP, NX)), dma((NP, NX)), dma((NZ,)), dma((NZ,)), dma((NZ,)), dma((NZ,)),
        ],
        compiler_params=pltpu.CompilerParams(collective_id=0, has_side_effects=True),
        name="exchange",
    )(row_block, coulomb.reshape(1, G), density)
    return out.reshape(1, 64, 2, RB)


def solution(mesh):
    return jax.shard_map(
        body,
        mesh=mesh,
        in_specs=(P(None, "ga", "ta"), P("ga"), P()),
        out_specs=P("ta", "ga", None, None),
        check_vma=False,
    )
```

```python
import jax
import jax.numpy as jnp
from jax import lax
from jax.experimental import pallas as pl
from jax.experimental.pallas import tpu as pltpu
from jax.sharding import PartitionSpec as P

MESH = pl.DeviceIdType.MESH
RB = 240
RBP = 256
G = 96
COLS = 4096
WIN = 384
NX, NY, NZ = 4, 2, 8
Q = 48
ORDER = ((2, 1), (2, 0), (3, 1), (1, 1), (3, 0), (1, 0), (0, 1), (0, 0))
NP = len(ORDER)
SUMS = {4: (2,), 5: (3,), 6: (1,), 7: (0,)}
EARLY = 1


def place(x, yh, z, yl, c):
    return (yh * (NZ * NX) + z * NX + x, yl * 2 + c)


def kernel(row_hbm, coul_hbm, dens_ref, out_ref, row_ref, coul_ref, dv, wpart, s1buf, fbuf, spare, fstack, sbuf, dbuf, csend, crecv, keep, zsend, zrecv,
           lsem, ready, s1s, s1r, fs, fr, ts, tr, ds, dr, cs, cr, zs, zr):
    ga = lax.axis_index("ga")
    ta = lax.axis_index("ta")
    x, z, yh = ga % NX, (ga // NX) % NZ, ga // (NX * NZ)
    yl, c = ta // 2, ta % 2
    kz, par = z // 2, z % 2

    loads = [pltpu.make_async_copy(a, b, lsem.at[i])
             for i, (a, b) in enumerate(((dens_ref, dv), (row_hbm, row_ref), (coul_hbm, coul_ref)))]
    for load in loads:
        load.start()

    def pair(m):
        a, b = kz // 2, kz % 2
        return (a + m // 2) % 2 * 2 + (b + m % 2) % 2

    def beside(r):
        return place((x + r) % NX, yh, z, yl, c)

    def along(m):
        return place(x, yh, 2 * pair(m) + par, yl, c)

    def square(e):
        return place(x, (yh + e // 2) % NY, 2 * kz + (par + e % 2) % 2, yl, c)

    def mates(q):
        return ((yl + q // 2) % 2, (c + q % 2) % 2)

    twin = place(x, yh, z, yl, (c + 1) % 2)

    bar = pltpu.get_barrier_semaphore()
    peers = [square(2), square(3)] + [place(x, yh, z, *mates(q)) for q in range(1, 4)]
    peers += [place((x + r) % NX, yh, z, (yl + u) % 2, c) for r in range(1, NX) for u in range(2)]
    for peer in peers:
        pl.semaphore_signal(bar, inc=1, device_id=peer, device_id_type=MESH)

    def greet(sem, d):
        @pl.when(z + d < NZ)
        def _():
            pl.semaphore_signal(sem, inc=1, device_id=place(x, yh, z + d, yl, c), device_id_type=MESH)

        @pl.when(z >= d)
        def _():
            pl.semaphore_signal(sem, inc=1, device_id=place(x, yh, z - d, yl, c), device_id_type=MESH)

    def met(d):
        return jnp.where(z + d < NZ, 1, 0) + jnp.where(z >= d, 1, 0)

    greet(bar, 1)

    with jax.named_scope("load_wait"):
        for load in loads:
            load.wait()

    start = row_ref[0] * RB - ta * COLS
    tile = jnp.minimum(jnp.maximum(lax.shift_right_arithmetic(start, 7), 0), (COLS - WIN) // 128)
    src = lax.broadcasted_iota(jnp.int32, (WIN, RBP), 0) + tile * 128
    dst = lax.broadcasted_iota(jnp.int32, (WIN, RBP), 1)
    hit = jnp.logical_and(src == dst + start, dst < RB)
    onehot = jnp.where(hit, 1.0, 0.0).astype(jnp.bfloat16)
    diag = lax.broadcasted_iota(jnp.int32, (G, G), 0) == lax.broadcasted_iota(jnp.int32, (G, G), 1)
    weight = jnp.sum(jnp.where(diag, jnp.broadcast_to(coul_ref[...], (G, G)), 0.0), axis=1, keepdims=True)
    for part in range(2):
        window = dv[part, :, :WIN]
        for k in range(1, (COLS - WIN) // 128 + 1):
            window = jnp.where(tile == k, dv[part, :, k * 128:k * 128 + WIN], window)
        picked = jnp.dot(window, onehot, preferred_element_type=jnp.float32)
        weighted = (weight * picked).astype(jnp.bfloat16)
        wpart[2 * part] = weighted[:Q]
        wpart[2 * part + 1] = weighted[Q:]

    low = lax.broadcasted_iota(jnp.int32, (G, 128), 1) < 64

    def pack(p):
        delta, w = ORDER[p]
        y = (yh + w) % NY
        zpair = 2 * pair(delta)
        z0 = zpair + par
        z1 = zpair + (par + 1) % 2
        for part in range(2):
            for h in range(2):
                o0 = pl.multiple_of((y * 16 + z0 * 2 + h) * 128, 128)
                o1 = pl.multiple_of((y * 16 + z1 * 2 + h) * 128, 128)
                t0 = dv[part, :, pl.ds(o0, 128)].astype(jnp.float32)
                t1 = dv[part, :, pl.ds(o1, 128)].astype(jnp.float32)
                even = jnp.where(low, t0, pltpu.roll(t1, 64, 1))
                odd = jnp.where(low, pltpu.roll(t0, 64, 1), t1)
                sbuf[p, 2 * h, part * G:(part + 1) * G, :] = even.astype(jnp.bfloat16)
                sbuf[p, 2 * h + 1, part * G:(part + 1) * G, :] = odd.astype(jnp.bfloat16)
        dbuf[p, 0] = sbuf[p, x]

    def send(src, dst, ss, rs, device):
        pltpu.make_async_remote_copy(src_ref=src, dst_ref=dst, send_sem=ss, recv_sem=rs, device_id=device,
                                     device_id_type=MESH).start()

    def wait(ref, sem):
        pltpu.make_async_copy(ref, ref, sem).wait()

    def spread(p):
        for r in range(1, NX):
            send(sbuf.at[p, (x + r) % NX], dbuf.at[p, r], ds, dr.at[p], beside(r))

    with jax.named_scope("pack0"):
        pack(0)
    with jax.named_scope("bar_wait"):
        pl.semaphore_wait(bar, len(peers) + met(1))

    for q in range(1, 4):
        ylq, cq = mates(q)
        send(wpart.at[ylq * 2 + cq], s1buf.at[q - 1], s1s, s1r, place(x, yh, z, ylq, cq))
    for p in range(EARLY):
        if p > 0:
            pack(p)
        spread(p)
    greet(ready.at[0], 1)
    with jax.named_scope("packs"):
        for p in range(EARLY, NP):
            pack(p)
    with jax.named_scope("ready0"):
        pl.semaphore_wait(ready.at[0], met(1))
    greet(ready.at[1], 2)
    with jax.named_scope("s1_wait"):
        wait(s1buf, s1r)
    total = wpart[ta].astype(jnp.float32)
    for q in range(3):
        total = total + s1buf[q].astype(jnp.float32)
    fbuf[0, yl, c] = total.astype(jnp.bfloat16)
    mine = fbuf.at[0, yl, c]
    for n in range(1, 2 * NX):
        r, u = n // 2, n % 2
        send(mine, fbuf.at[r, yl, c], fs, fr, place((x + r) % NX, yh, z, (yl + u) % 2, c))
    for p in range(EARLY, NP):
        spread(p)
    with jax.named_scope("ready1"):
        pl.semaphore_wait(ready.at[1], met(2))
    greet(ready.at[2], 4)
    with jax.named_scope("rows_wait"):
        wait(spare.at[0:2 * NX - 1], fr)
    send(fbuf.at[:, :, c], fbuf.at[:, :, c], ts, tr, twin)
    with jax.named_scope("across_wait"):
        wait(spare, tr)
    for r in range(NX):
        re = fbuf[r, 0].reshape(G, RBP)
        im = fbuf[r, 1].reshape(G, RBP)
        fstack[r * 2 * G:r * 2 * G + G, :RBP] = re
        fstack[r * 2 * G:r * 2 * G + G, RBP:] = -im
        fstack[r * 2 * G + G:(r + 1) * 2 * G, :RBP] = im
        fstack[r * 2 * G + G:(r + 1) * 2 * G, RBP:] = re


    def consume(m):
        with jax.named_scope(f"square_wait{m}"):
            wait(crecv.at[m, 1:4], cr.at[m])
        block = keep[m]
        for e in range(1, 4):
            block = block + crecv[m, e].astype(jnp.float32)
        if m == 0:
            return block
        if m == ORDER[0][0]:
            with jax.named_scope("ready2"):
                pl.semaphore_wait(ready.at[2], met(4))
        zsend[m] = block.astype(jnp.bfloat16)
        send(zsend.at[m], zrecv.at[m], zs, zr, along(m))
        return None

    for p, (m, w) in enumerate(ORDER):
        with jax.named_scope(f"piece_wait{p}"):
            wait(dbuf.at[p, 1:NX], dr.at[p])
        cols = dbuf[p].reshape(NX * 2 * G, 128)
        prod = lax.dot_general(cols, fstack[...], (((0,), (0,)), ((), ())), preferred_element_type=jnp.float32)
        for e in (2 * w + 1, 2 * w):
            block = prod[e % 2 * 64:(e % 2 + 1) * 64]
            if e == 0:
                keep[m] = block
            else:
                csend[m, e] = block.astype(jnp.bfloat16)
                send(csend.at[m, e], crecv.at[m, e], cs, cr.at[m], square(e))
        for done in SUMS.get(p, ()):
            acc = consume(done)
    with jax.named_scope("zwait"):
        wait(zrecv.at[1:4], zr)
    for m in range(1, 4):
        acc = acc + zrecv[m].astype(jnp.float32)
    out_ref[:, 0, :] = acc[:, :RB]
    out_ref[:, 1, :] = acc[:, RBP:RBP + RB]
    with jax.named_scope("send_waits"):
        wait(s1buf, s1s)
        wait(spare.at[0:2 * NX - 1], fs)
        wait(spare, ts)
        wait(dbuf.at[:, 1:NX], ds)
        wait(csend.at[:, 1:4], cs)
        wait(zsend.at[1:4], zs)


def body(density, coulomb, row_block):
    dma = pltpu.SemaphoreType.DMA
    bf16, f32 = jnp.bfloat16, jnp.float32
    out = pl.pallas_call(
        kernel,
        out_shape=pltpu.VMEM((64, 2, RB), f32),
        in_specs=[pl.BlockSpec(memory_space=pltpu.HBM)] * 3,
        out_specs=pl.BlockSpec(memory_space=pltpu.VMEM),
        scratch_shapes=[
            pltpu.SMEM((1,), jnp.int32),
            pltpu.VMEM((1, G), f32),
            pltpu.VMEM((2, G, COLS), bf16),
            pltpu.VMEM((4, Q, RBP), bf16),
            pltpu.VMEM((3, Q, RBP), bf16),
            pltpu.VMEM((NX, 2, 2, Q, RBP), bf16),
            pltpu.VMEM((2 * NX, Q, RBP), bf16),
            pltpu.VMEM((NX * 2 * G, 2 * RBP), bf16),
            pltpu.VMEM((NP, NX, 2 * G, 128), bf16),
            pltpu.VMEM((NP, NX, 2 * G, 128), bf16),
            pltpu.VMEM((4, 4, 64, 2 * RBP), bf16),
            pltpu.VMEM((4, 4, 64, 2 * RBP), bf16),
            pltpu.VMEM((4, 64, 2 * RBP), f32),
            pltpu.VMEM((4, 64, 2 * RBP), bf16),
            pltpu.VMEM((4, 64, 2 * RBP), bf16),
            dma((3,)), pltpu.SemaphoreType.REGULAR((3,)), dma, dma, dma, dma, dma, dma,
            dma, dma((NP,)), dma, dma((4,)), dma, dma,
        ],
        compiler_params=pltpu.CompilerParams(collective_id=0, has_side_effects=True),
        name="exchange",
    )(row_block, coulomb.reshape(1, G), density)
    return out.reshape(1, 64, 2, RB)


def solution(mesh):
    return jax.shard_map(
        body,
        mesh=mesh,
        in_specs=(P(None, "ga", "ta"), P("ga"), P()),
        out_specs=P("ta", "ga", None, None),
        check_vma=False,
    )
```

```python
import jax
import jax.numpy as jnp
from jax import lax
from jax.experimental import pallas as pl
from jax.experimental.pallas import tpu as pltpu
from jax.sharding import PartitionSpec as P

MESH = pl.DeviceIdType.MESH
RB = 240
RBP = 256
G = 96
COLS = 4096
WIN = 384
NX, NY, NZ = 4, 2, 8
Q = 48
ORDER = ((2, 1), (2, 0), (1, 1), (3, 1), (3, 0), (1, 0), (0, 1), (0, 0))
NP = len(ORDER)
SUMS = {4: (2,), 5: (3,), 6: (1,), 7: (0,)}
EARLY = 1


def place(x, yh, z, yl, c):
    return (yh * (NZ * NX) + z * NX + x, yl * 2 + c)


def kernel(row_hbm, coul_hbm, dens_ref, out_ref, row_ref, coul_ref, dv, wpart, s1buf, fbuf, spare, fstack, sbuf, dbuf, csend, crecv, keep, zsend, zrecv,
           lsem, ready, s1s, s1r, fs, fr, ts, tr, ds, dr, cs, cr, zs, zr):
    ga = lax.axis_index("ga")
    ta = lax.axis_index("ta")
    x, z, yh = ga % NX, (ga // NX) % NZ, ga // (NX * NZ)
    yl, c = ta // 2, ta % 2
    kz, par = z // 2, z % 2

    loads = [pltpu.make_async_copy(a, b, lsem.at[i])
             for i, (a, b) in enumerate(((dens_ref, dv), (row_hbm, row_ref), (coul_hbm, coul_ref)))]
    for load in loads:
        load.start()

    def pair(m):
        a, b = kz // 2, kz % 2
        return (a + m // 2) % 2 * 2 + (b + m % 2) % 2

    def beside(r):
        return place((x + r) % NX, yh, z, yl, c)

    def along(m):
        return place(x, yh, 2 * pair(m) + par, yl, c)

    def square(e):
        return place(x, (yh + e // 2) % NY, 2 * kz + (par + e % 2) % 2, yl, c)

    def mates(q):
        return ((yl + q // 2) % 2, (c + q % 2) % 2)

    twin = place(x, yh, z, yl, (c + 1) % 2)

    bar = pltpu.get_barrier_semaphore()
    peers = [square(2), square(3)] + [place(x, yh, z, *mates(q)) for q in range(1, 4)]
    peers += [place((x + r) % NX, yh, z, (yl + u) % 2, c) for r in range(1, NX) for u in range(2)]
    for peer in peers:
        pl.semaphore_signal(bar, inc=1, device_id=peer, device_id_type=MESH)

    def greet(sem, d):
        @pl.when(z + d < NZ)
        def _():
            pl.semaphore_signal(sem, inc=1, device_id=place(x, yh, z + d, yl, c), device_id_type=MESH)

        @pl.when(z >= d)
        def _():
            pl.semaphore_signal(sem, inc=1, device_id=place(x, yh, z - d, yl, c), device_id_type=MESH)

    def met(d):
        return jnp.where(z + d < NZ, 1, 0) + jnp.where(z >= d, 1, 0)

    greet(bar, 1)

    with jax.named_scope("load_wait"):
        for load in loads:
            load.wait()

    start = row_ref[0] * RB - ta * COLS
    tile = jnp.minimum(jnp.maximum(lax.shift_right_arithmetic(start, 7), 0), (COLS - WIN) // 128)
    src = lax.broadcasted_iota(jnp.int32, (WIN, RBP), 0) + tile * 128
    dst = lax.broadcasted_iota(jnp.int32, (WIN, RBP), 1)
    hit = jnp.logical_and(src == dst + start, dst < RB)
    onehot = jnp.where(hit, 1.0, 0.0).astype(jnp.bfloat16)
    diag = lax.broadcasted_iota(jnp.int32, (G, G), 0) == lax.broadcasted_iota(jnp.int32, (G, G), 1)
    weight = jnp.sum(jnp.where(diag, jnp.broadcast_to(coul_ref[...], (G, G)), 0.0), axis=1, keepdims=True)
    for part in range(2):
        window = dv[part, :, :WIN]
        for k in range(1, (COLS - WIN) // 128 + 1):
            window = jnp.where(tile == k, dv[part, :, k * 128:k * 128 + WIN], window)
        picked = jnp.dot(window, onehot, preferred_element_type=jnp.float32)
        weighted = (weight * picked).astype(jnp.bfloat16)
        wpart[2 * part] = weighted[:Q]
        wpart[2 * part + 1] = weighted[Q:]

    low = lax.broadcasted_iota(jnp.int32, (G, 128), 1) < 64

    def pack(p):
        delta, w = ORDER[p]
        y = (yh + w) % NY
        zpair = 2 * pair(delta)
        z0 = zpair + par
        z1 = zpair + (par + 1) % 2
        for part in range(2):
            for h in range(2):
                o0 = pl.multiple_of((y * 16 + z0 * 2 + h) * 128, 128)
                o1 = pl.multiple_of((y * 16 + z1 * 2 + h) * 128, 128)
                t0 = dv[part, :, pl.ds(o0, 128)].astype(jnp.float32)
                t1 = dv[part, :, pl.ds(o1, 128)].astype(jnp.float32)
                even = jnp.where(low, t0, pltpu.roll(t1, 64, 1))
                odd = jnp.where(low, pltpu.roll(t0, 64, 1), t1)
                sbuf[p, 2 * h, part * G:(part + 1) * G, :] = even.astype(jnp.bfloat16)
                sbuf[p, 2 * h + 1, part * G:(part + 1) * G, :] = odd.astype(jnp.bfloat16)
        dbuf[p, 0] = sbuf[p, x]

    def send(src, dst, ss, rs, device):
        pltpu.make_async_remote_copy(src_ref=src, dst_ref=dst, send_sem=ss, recv_sem=rs, device_id=device,
                                     device_id_type=MESH).start()

    def wait(ref, sem):
        pltpu.make_async_copy(ref, ref, sem).wait()

    def spread(p):
        for r in range(1, NX):
            send(sbuf.at[p, (x + r) % NX], dbuf.at[p, r], ds, dr.at[p], beside(r))

    with jax.named_scope("pack0"):
        pack(0)
    with jax.named_scope("bar_wait"):
        pl.semaphore_wait(bar, len(peers) + met(1))

    for q in range(1, 4):
        ylq, cq = mates(q)
        send(wpart.at[ylq * 2 + cq], s1buf.at[q - 1], s1s, s1r, place(x, yh, z, ylq, cq))
    for p in range(EARLY):
        if p > 0:
            pack(p)
        spread(p)
    greet(ready.at[0], 1)
    with jax.named_scope("packs"):
        for p in range(EARLY, NP):
            pack(p)
    with jax.named_scope("ready0"):
        pl.semaphore_wait(ready.at[0], met(1))
    greet(ready.at[1], 2)
    with jax.named_scope("s1_wait"):
        wait(s1buf, s1r)
    total = wpart[ta].astype(jnp.float32)
    for q in range(3):
        total = total + s1buf[q].astype(jnp.float32)
    fbuf[0, yl, c] = total.astype(jnp.bfloat16)
    mine = fbuf.at[0, yl, c]
    for n in range(1, 2 * NX):
        r, u = n // 2, n % 2
        send(mine, fbuf.at[r, yl, c], fs, fr, place((x + r) % NX, yh, z, (yl + u) % 2, c))
    for p in range(EARLY, NP):
        spread(p)
    with jax.named_scope("ready1"):
        pl.semaphore_wait(ready.at[1], met(2))
    greet(ready.at[2], 4)
    with jax.named_scope("rows_wait"):
        wait(spare.at[0:2 * NX - 1], fr)
    send(fbuf.at[:, :, c], fbuf.at[:, :, c], ts, tr, twin)
    with jax.named_scope("across_wait"):
        wait(spare, tr)
    for r in range(NX):
        re = fbuf[r, 0].reshape(G, RBP)
        im = fbuf[r, 1].reshape(G, RBP)
        fstack[r * 2 * G:r * 2 * G + G, :RBP] = re
        fstack[r * 2 * G:r * 2 * G + G, RBP:] = -im
        fstack[r * 2 * G + G:(r + 1) * 2 * G, :RBP] = im
        fstack[r * 2 * G + G:(r + 1) * 2 * G, RBP:] = re


    def consume(m):
        with jax.named_scope(f"square_wait{m}"):
            wait(crecv.at[m, 1:4], cr.at[m])
        block = keep[m]
        for e in range(1, 4):
            block = block + crecv[m, e].astype(jnp.float32)
        if m == 0:
            return block
        if m == ORDER[0][0]:
            with jax.named_scope("ready2"):
                pl.semaphore_wait(ready.at[2], met(4))
        zsend[m] = block.astype(jnp.bfloat16)
        send(zsend.at[m], zrecv.at[m], zs, zr, along(m))
        return None

    for p, (m, w) in enumerate(ORDER):
        with jax.named_scope(f"piece_wait{p}"):
            wait(dbuf.at[p, 1:NX], dr.at[p])
        cols = dbuf[p].reshape(NX * 2 * G, 128)
        prod = lax.dot_general(cols, fstack[...], (((0,), (0,)), ((), ())), preferred_element_type=jnp.float32)
        for e in (2 * w + 1, 2 * w):
            block = prod[e % 2 * 64:(e % 2 + 1) * 64]
            if e == 0:
                keep[m] = block
            else:
                csend[m, e] = block.astype(jnp.bfloat16)
                send(csend.at[m, e], crecv.at[m, e], cs, cr.at[m], square(e))
        for done in SUMS.get(p, ()):
            acc = consume(done)
    with jax.named_scope("zwait"):
        wait(zrecv.at[1:4], zr)
    for m in range(1, 4):
        acc = acc + zrecv[m].astype(jnp.float32)
    out_ref[:, 0, :] = acc[:, :RB]
    out_ref[:, 1, :] = acc[:, RBP:RBP + RB]
    with jax.named_scope("send_waits"):
        wait(s1buf, s1s)
        wait(spare.at[0:2 * NX - 1], fs)
        wait(spare, ts)
        wait(dbuf.at[:, 1:NX], ds)
        wait(csend.at[:, 1:4], cs)
        wait(zsend.at[1:4], zs)


def body(density, coulomb, row_block):
    dma = pltpu.SemaphoreType.DMA
    bf16, f32 = jnp.bfloat16, jnp.float32
    out = pl.pallas_call(
        kernel,
        out_shape=pltpu.VMEM((64, 2, RB), f32),
        in_specs=[pl.BlockSpec(memory_space=pltpu.HBM)] * 3,
        out_specs=pl.BlockSpec(memory_space=pltpu.VMEM),
        scratch_shapes=[
            pltpu.SMEM((1,), jnp.int32),
            pltpu.VMEM((1, G), f32),
            pltpu.VMEM((2, G, COLS), bf16),
            pltpu.VMEM((4, Q, RBP), bf16),
            pltpu.VMEM((3, Q, RBP), bf16),
            pltpu.VMEM((NX, 2, 2, Q, RBP), bf16),
            pltpu.VMEM((2 * NX, Q, RBP), bf16),
            pltpu.VMEM((NX * 2 * G, 2 * RBP), bf16),
            pltpu.VMEM((NP, NX, 2 * G, 128), bf16),
            pltpu.VMEM((NP, NX, 2 * G, 128), bf16),
            pltpu.VMEM((4, 4, 64, 2 * RBP), bf16),
            pltpu.VMEM((4, 4, 64, 2 * RBP), bf16),
            pltpu.VMEM((4, 64, 2 * RBP), f32),
            pltpu.VMEM((4, 64, 2 * RBP), bf16),
            pltpu.VMEM((4, 64, 2 * RBP), bf16),
            dma((3,)), pltpu.SemaphoreType.REGULAR((3,)), dma, dma, dma, dma, dma, dma,
            dma, dma((NP,)), dma, dma((4,)), dma, dma,
        ],
        compiler_params=pltpu.CompilerParams(collective_id=0, has_side_effects=True),
        name="exchange",
    )(row_block, coulomb.reshape(1, G), density)
    return out.reshape(1, 64, 2, RB)


def solution(mesh):
    return jax.shard_map(
        body,
        mesh=mesh,
        in_specs=(P(None, "ga", "ta"), P("ga"), P()),
        out_specs=P("ta", "ga", None, None),
        check_vma=False,
    )
```

```python
import jax
import jax.numpy as jnp
from jax import lax
from jax.experimental import pallas as pl
from jax.experimental.pallas import tpu as pltpu
from jax.sharding import PartitionSpec as P

MESH = pl.DeviceIdType.MESH
RB = 240
RBP = 256
G = 96
COLS = 4096
WIN = 384
NX, NY, NZ = 4, 2, 8
FAR = (2, 1, 3)
STEPS = ("O2", "W2", "O1", "O3", "W3", "C2", "W1", "C3", "O0", "C1", "W0", "C0")
VIA = {2: 1, 3: 3, 1: 1}
ORDER = tuple((int(step[1]), int(step[0] == "O")) for step in STEPS if step[0] in "OW")
NP = len(ORDER)
EARLY = 2


def place(x, yh, z, yl, c):
    return (yh * (NZ * NX) + z * NX + x, yl * 2 + c)


def kernel(row_hbm, coul_hbm, dens_ref, out_ref, row_ref, coul_ref, dv, wpart, s1buf, fbuf, spare, fstack, sbuf, dbuf, csend, crecv, keep, zsend, zrecv,
           lsem, ready, s1s, s1r, fs, fr, ts, tr, ds, dr, cs, cr, zs, zr):
    ga = lax.axis_index("ga")
    ta = lax.axis_index("ta")
    x, z, yh = ga % NX, (ga // NX) % NZ, ga // (NX * NZ)
    yl, c = ta // 2, ta % 2
    kz, par = z // 2, z % 2

    loads = [pltpu.make_async_copy(a, b, lsem.at[i])
             for i, (a, b) in enumerate(((dens_ref, dv), (row_hbm, row_ref), (coul_hbm, coul_ref)))]
    for load in loads:
        load.start()

    def pair(m):
        a, b = kz // 2, kz % 2
        return (a + m // 2) % 2 * 2 + (b + m % 2) % 2

    def beside(r):
        return place((x + r) % NX, yh, z, yl, c)

    def along(m):
        return place(x, yh, 2 * pair(m) + par, yl, c)

    def square(e):
        return place(x, (yh + e // 2) % NY, 2 * kz + (par + e % 2) % 2, yl, c)

    def mates(q):
        return ((yl + q // 2) % 2, (c + q % 2) % 2)

    twin = place(x, yh, z, yl, (c + 1) % 2)

    bar = pltpu.get_barrier_semaphore()
    peers = [square(2), square(3)] + [place(x, yh, z, *mates(q)) for q in range(1, 4)]
    peers += [beside(r) for r in range(1, NX)]
    for peer in peers:
        pl.semaphore_signal(bar, inc=1, device_id=peer, device_id_type=MESH)

    def greet(sem, d):
        @pl.when(z + d < NZ)
        def _():
            pl.semaphore_signal(sem, inc=1, device_id=place(x, yh, z + d, yl, c), device_id_type=MESH)

        @pl.when(z >= d)
        def _():
            pl.semaphore_signal(sem, inc=1, device_id=place(x, yh, z - d, yl, c), device_id_type=MESH)

    def met(d):
        return jnp.where(z + d < NZ, 1, 0) + jnp.where(z >= d, 1, 0)

    greet(bar, 1)

    with jax.named_scope("load_wait"):
        for load in loads:
            load.wait()

    start = row_ref[0] * RB - ta * COLS
    tile = jnp.minimum(jnp.maximum(lax.shift_right_arithmetic(start, 7), 0), (COLS - WIN) // 128)
    src = lax.broadcasted_iota(jnp.int32, (WIN, RBP), 0) + tile * 128
    dst = lax.broadcasted_iota(jnp.int32, (WIN, RBP), 1)
    hit = jnp.logical_and(src == dst + start, dst < RB)
    onehot = jnp.where(hit, 1.0, 0.0).astype(jnp.bfloat16)
    diag = lax.broadcasted_iota(jnp.int32, (G, G), 0) == lax.broadcasted_iota(jnp.int32, (G, G), 1)
    weight = jnp.sum(jnp.where(diag, jnp.broadcast_to(coul_ref[...], (G, G)), 0.0), axis=1, keepdims=True)
    for part in range(2):
        window = dv[part, :, :WIN]
        for k in range(1, (COLS - WIN) // 128 + 1):
            window = jnp.where(tile == k, dv[part, :, k * 128:k * 128 + WIN], window)
        picked = jnp.dot(window, onehot, preferred_element_type=jnp.float32)
        wpart[part] = (weight * picked).astype(jnp.bfloat16)

    low = lax.broadcasted_iota(jnp.int32, (G, 128), 1) < 64

    def pack(p):
        delta, w = ORDER[p]
        y = (yh + w) % NY
        zpair = 2 * pair(delta)
        z0 = zpair + par
        z1 = zpair + (par + 1) % 2
        for part in range(2):
            for h in range(2):
                o0 = pl.multiple_of((y * 16 + z0 * 2 + h) * 128, 128)
                o1 = pl.multiple_of((y * 16 + z1 * 2 + h) * 128, 128)
                t0 = dv[part, :, pl.ds(o0, 128)].astype(jnp.float32)
                t1 = dv[part, :, pl.ds(o1, 128)].astype(jnp.float32)
                even = jnp.where(low, t0, pltpu.roll(t1, 64, 1))
                odd = jnp.where(low, pltpu.roll(t0, 64, 1), t1)
                sbuf[p, 2 * h, part * G:(part + 1) * G, :] = even.astype(jnp.bfloat16)
                sbuf[p, 2 * h + 1, part * G:(part + 1) * G, :] = odd.astype(jnp.bfloat16)
        dbuf[p, 0] = sbuf[p, x]

    def send(src, dst, ss, rs, device):
        pltpu.make_async_remote_copy(src_ref=src, dst_ref=dst, send_sem=ss, recv_sem=rs, device_id=device,
                                     device_id_type=MESH).start()

    def wait(ref, sem):
        pltpu.make_async_copy(ref, ref, sem).wait()

    def spread(p):
        for r in range(1, NX):
            send(sbuf.at[p, (x + r) % NX], dbuf.at[p, r], ds, dr.at[p], beside(r))

    with jax.named_scope("pack0"):
        pack(0)
    with jax.named_scope("bar_wait"):
        pl.semaphore_wait(bar, len(peers) + met(1))

    for q in range(1, 4):
        ylq, cq = mates(q)
        send(wpart.at[cq], s1buf.at[q - 1], s1s, s1r, place(x, yh, z, ylq, cq))
    for p in range(EARLY):
        if p > 0:
            pack(p)
        spread(p)
    greet(ready.at[0], 1)
    with jax.named_scope("packs"):
        for p in range(EARLY, NP):
            pack(p)
    with jax.named_scope("ready0"):
        pl.semaphore_wait(ready.at[0], met(1))
    greet(ready.at[1], 2)
    with jax.named_scope("s1_wait"):
        wait(s1buf, s1r)
    total = wpart[c].astype(jnp.float32)
    for q in range(3):
        total = total + s1buf[q].astype(jnp.float32)
    fbuf[0, c] = total.astype(jnp.bfloat16)
    for r in FAR:
        send(fbuf.at[0, c], fbuf.at[r, c], fs, fr, beside(r))
    wait(spare.at[1:NX], fs)
    for p in range(EARLY, NP):
        spread(p)
    with jax.named_scope("ready1"):
        pl.semaphore_wait(ready.at[1], met(2))
    greet(ready.at[2], 4)
    with jax.named_scope("rows_wait"):
        wait(spare.at[1:NX], fr)
    send(fbuf.at[:, c], fbuf.at[:, c], ts, tr, twin)
    with jax.named_scope("across_wait"):
        wait(spare, tr)
    for r in range(NX):
        re = fbuf[r, 0].astype(jnp.float32)[:, :RB]
        im = fbuf[r, 1].astype(jnp.float32)[:, :RB]
        none = jnp.zeros((G, 2 * (RBP - RB)), jnp.float32)
        fstack[r * 2 * G:r * 2 * G + G] = jnp.concatenate([re, -im, none], axis=1).astype(jnp.bfloat16)
        fstack[r * 2 * G + G:(r + 1) * 2 * G] = jnp.concatenate([im, re, none], axis=1).astype(jnp.bfloat16)

    lane = lax.broadcasted_iota(jnp.int32, (16, 128), 1)

    def packed(block):
        tail = block[:, 384:]
        rest = [jnp.where(lane < 96, tail[16 * j:16 * j + 16], pltpu.roll(tail[48:], 96 - 32 * j, 1)) for j in range(3)]
        return jnp.concatenate([block[:, :128], block[:, 128:256], block[:, 256:384], *rest], axis=0)

    def unpacked(block):
        rest = [block[192 + 16 * j:208 + 16 * j] for j in range(3)]
        back = [pltpu.roll(rest[j], 32 * j + 32, 1) for j in range(3)]
        last = jnp.where(lane < 32, back[0], jnp.where(lane < 64, back[1], back[2]))
        tail = jnp.concatenate([*rest, last], axis=0)
        return jnp.concatenate([block[:64], block[64:128], block[128:192], tail], axis=1)

    def produce(p):
        m, w = ORDER[p]
        with jax.named_scope(f"piece_wait{p}"):
            wait(dbuf.at[p, 1:NX], dr.at[p])
        cols = dbuf[p].reshape(NX * 2 * G, 128)
        prod = lax.dot_general(cols, fstack[...], (((0,), (0,)), ((), ())), preferred_element_type=jnp.float32)
        for e in (2 * w + 1, 2 * w):
            block = packed(prod[e % 2 * 64:(e % 2 + 1) * 64])
            if e == 0:
                keep[m] = block
            else:
                csend[m, e] = block.astype(jnp.bfloat16)
                send(csend.at[m, e], crecv.at[m, e], cs, cr.at[m, e], square(e))

    def consume(m):
        block = keep[m]
        for e in (2, 1, 3):
            with jax.named_scope(f"square_wait{m}"):
                wait(crecv.at[m, e], cr.at[m, e])
            block = block + crecv[m, e].astype(jnp.float32)
        if m == 0:
            return block
        if m == 3:
            with jax.named_scope("via_wait"):
                wait(zrecv.at[2], zr.at[2])
            block = block + zrecv[2].astype(jnp.float32)
        zsend[m] = block.astype(jnp.bfloat16)
        send(zsend.at[m], zrecv.at[m], zs, zr.at[m], along(VIA[m]))
        return None

    piece = 0
    greeted = False
    for step in STEPS:
        m = int(step[1])
        if step[0] == "C":
            if not greeted:
                greeted = True
                with jax.named_scope("ready2"):
                    pl.semaphore_wait(ready.at[2], met(4))
            if m == 0:
                acc = consume(m)
            else:
                consume(m)
        else:
            produce(piece)
            piece += 1
    for m in (3, 1):
        with jax.named_scope(f"zwait{m}"):
            wait(zrecv.at[m], zr.at[m])
        acc = acc + zrecv[m].astype(jnp.float32)
    full = unpacked(acc)
    out_ref[:, 0, :] = full[:, :RB]
    out_ref[:, 1, :] = pltpu.roll(full, 2 * RBP - RB, 1)[:, :RB]
    with jax.named_scope("send_waits"):
        wait(s1buf, s1s)
        wait(spare, ts)
        wait(dbuf.at[:, 1:NX], ds)
        wait(csend.at[:, 1:4], cs)
        wait(zsend.at[1:4], zs)


def body(density, coulomb, row_block):
    dma = pltpu.SemaphoreType.DMA
    bf16, f32 = jnp.bfloat16, jnp.float32
    out = pl.pallas_call(
        kernel,
        out_shape=pltpu.VMEM((64, 2, RB), f32),
        in_specs=[pl.BlockSpec(memory_space=pltpu.HBM)] * 3,
        out_specs=pl.BlockSpec(memory_space=pltpu.VMEM),
        scratch_shapes=[
            pltpu.SMEM((1,), jnp.int32),
            pltpu.VMEM((1, G), f32),
            pltpu.VMEM((2, G, COLS), bf16),
            pltpu.VMEM((2, G, RBP), bf16),
            pltpu.VMEM((3, G, RBP), bf16),
            pltpu.VMEM((NX, 2, G, RBP), bf16),
            pltpu.VMEM((NX, G, RBP), bf16),
            pltpu.VMEM((NX * 2 * G, 2 * RBP), bf16),
            pltpu.VMEM((NP, NX, 2 * G, 128), bf16),
            pltpu.VMEM((NP, NX, 2 * G, 128), bf16),
            pltpu.VMEM((4, 4, 240, 128), bf16),
            pltpu.VMEM((4, 4, 240, 128), bf16),
            pltpu.VMEM((4, 240, 128), f32),
            pltpu.VMEM((4, 240, 128), bf16),
            pltpu.VMEM((4, 240, 128), bf16),
            dma((3,)), pltpu.SemaphoreType.REGULAR((3,)), dma, dma, dma, dma, dma, dma,
            dma, dma((NP,)), dma, dma((4, 4)), dma, dma((4,)),
        ],
        compiler_params=pltpu.CompilerParams(collective_id=0, has_side_effects=True),
        name="exchange",
    )(row_block, coulomb.reshape(1, G), density)
    return out.reshape(1, 64, 2, RB)


def solution(mesh):
    return jax.shard_map(
        body,
        mesh=mesh,
        in_specs=(P(None, "ga", "ta"), P("ga"), P()),
        out_specs=P("ta", "ga", None, None),
        check_vma=False,
    )
```

```python
import jax
import jax.numpy as jnp
from jax import lax
from jax.experimental import pallas as pl
from jax.experimental.pallas import tpu as pltpu
from jax.sharding import PartitionSpec as P

MESH = pl.DeviceIdType.MESH
RB = 240
RBP = 256
G = 96
COLS = 4096
WIN = 384
NX, NY, NZ = 4, 2, 8
FAR = (2, 1, 3)
STEPS = ("O2", "W2", "O3", "O1", "W3", "C2", "W1", "C3", "O0", "C1", "W0", "C0")
VIA = {2: 1, 3: 3, 1: 1}
ORDER = tuple((int(step[1]), int(step[0] == "O")) for step in STEPS if step[0] in "OW")
NP = len(ORDER)
EARLY = 2


def place(x, yh, z, yl, c):
    return (yh * (NZ * NX) + z * NX + x, yl * 2 + c)


def kernel(row_hbm, coul_hbm, dens_ref, out_ref, row_ref, coul_ref, dv, wpart, s1buf, fbuf, spare, fstack, sbuf, dbuf, csend, crecv, keep, zsend, zrecv,
           lsem, ready, s1s, s1r, fs, fr, ts, tr, ds, dr, cs, cr, zs, zr):
    ga = lax.axis_index("ga")
    ta = lax.axis_index("ta")
    x, z, yh = ga % NX, (ga // NX) % NZ, ga // (NX * NZ)
    yl, c = ta // 2, ta % 2
    kz, par = z // 2, z % 2

    loads = [pltpu.make_async_copy(a, b, lsem.at[i])
             for i, (a, b) in enumerate(((dens_ref, dv), (row_hbm, row_ref), (coul_hbm, coul_ref)))]
    for load in loads:
        load.start()

    def pair(m):
        a, b = kz // 2, kz % 2
        return (a + m // 2) % 2 * 2 + (b + m % 2) % 2

    def beside(r):
        return place((x + r) % NX, yh, z, yl, c)

    def along(m):
        return place(x, yh, 2 * pair(m) + par, yl, c)

    def square(e):
        return place(x, (yh + e // 2) % NY, 2 * kz + (par + e % 2) % 2, yl, c)

    def mates(q):
        return ((yl + q // 2) % 2, (c + q % 2) % 2)

    twin = place(x, yh, z, yl, (c + 1) % 2)

    bar = pltpu.get_barrier_semaphore()
    peers = [square(2), square(3)] + [place(x, yh, z, *mates(q)) for q in range(1, 4)]
    peers += [beside(r) for r in range(1, NX)]
    for peer in peers:
        pl.semaphore_signal(bar, inc=1, device_id=peer, device_id_type=MESH)

    def greet(sem, d):
        @pl.when(z + d < NZ)
        def _():
            pl.semaphore_signal(sem, inc=1, device_id=place(x, yh, z + d, yl, c), device_id_type=MESH)

        @pl.when(z >= d)
        def _():
            pl.semaphore_signal(sem, inc=1, device_id=place(x, yh, z - d, yl, c), device_id_type=MESH)

    def met(d):
        return jnp.where(z + d < NZ, 1, 0) + jnp.where(z >= d, 1, 0)

    greet(bar, 1)

    with jax.named_scope("load_wait"):
        for load in loads:
            load.wait()

    start = row_ref[0] * RB - ta * COLS
    tile = jnp.minimum(jnp.maximum(lax.shift_right_arithmetic(start, 7), 0), (COLS - WIN) // 128)
    src = lax.broadcasted_iota(jnp.int32, (WIN, RBP), 0) + tile * 128
    dst = lax.broadcasted_iota(jnp.int32, (WIN, RBP), 1)
    hit = jnp.logical_and(src == dst + start, dst < RB)
    onehot = jnp.where(hit, 1.0, 0.0).astype(jnp.bfloat16)
    diag = lax.broadcasted_iota(jnp.int32, (G, G), 0) == lax.broadcasted_iota(jnp.int32, (G, G), 1)
    weight = jnp.sum(jnp.where(diag, jnp.broadcast_to(coul_ref[...], (G, G)), 0.0), axis=1, keepdims=True)
    for part in range(2):
        window = dv[part, :, :WIN]
        for k in range(1, (COLS - WIN) // 128 + 1):
            window = jnp.where(tile == k, dv[part, :, k * 128:k * 128 + WIN], window)
        picked = jnp.dot(window, onehot, preferred_element_type=jnp.float32)
        wpart[part] = (weight * picked).astype(jnp.bfloat16)

    low = lax.broadcasted_iota(jnp.int32, (G, 128), 1) < 64

    def pack(p):
        delta, w = ORDER[p]
        y = (yh + w) % NY
        zpair = 2 * pair(delta)
        z0 = zpair + par
        z1 = zpair + (par + 1) % 2
        for part in range(2):
            for h in range(2):
                o0 = pl.multiple_of((y * 16 + z0 * 2 + h) * 128, 128)
                o1 = pl.multiple_of((y * 16 + z1 * 2 + h) * 128, 128)
                t0 = dv[part, :, pl.ds(o0, 128)].astype(jnp.float32)
                t1 = dv[part, :, pl.ds(o1, 128)].astype(jnp.float32)
                even = jnp.where(low, t0, pltpu.roll(t1, 64, 1))
                odd = jnp.where(low, pltpu.roll(t0, 64, 1), t1)
                sbuf[p, 2 * h, part * G:(part + 1) * G, :] = even.astype(jnp.bfloat16)
                sbuf[p, 2 * h + 1, part * G:(part + 1) * G, :] = odd.astype(jnp.bfloat16)
        dbuf[p, 0] = sbuf[p, x]

    def send(src, dst, ss, rs, device):
        pltpu.make_async_remote_copy(src_ref=src, dst_ref=dst, send_sem=ss, recv_sem=rs, device_id=device,
                                     device_id_type=MESH).start()

    def wait(ref, sem):
        pltpu.make_async_copy(ref, ref, sem).wait()

    def spread(p):
        for r in range(1, NX):
            send(sbuf.at[p, (x + r) % NX], dbuf.at[p, r], ds, dr.at[p], beside(r))

    with jax.named_scope("pack0"):
        pack(0)
    with jax.named_scope("bar_wait"):
        pl.semaphore_wait(bar, len(peers) + met(1))

    for q in range(1, 4):
        ylq, cq = mates(q)
        send(wpart.at[cq], s1buf.at[q - 1], s1s, s1r, place(x, yh, z, ylq, cq))
    for p in range(EARLY):
        if p > 0:
            pack(p)
        spread(p)
    greet(ready.at[0], 1)
    with jax.named_scope("packs"):
        for p in range(EARLY, NP):
            pack(p)
    with jax.named_scope("ready0"):
        pl.semaphore_wait(ready.at[0], met(1))
    greet(ready.at[1], 2)
    with jax.named_scope("s1_wait"):
        wait(s1buf, s1r)
    total = wpart[c].astype(jnp.float32)
    for q in range(3):
        total = total + s1buf[q].astype(jnp.float32)
    fbuf[0, c] = total.astype(jnp.bfloat16)
    for r in FAR:
        send(fbuf.at[0, c], fbuf.at[r, c], fs, fr, beside(r))
    wait(spare.at[1:NX], fs)
    for p in range(EARLY, NP):
        spread(p)
    with jax.named_scope("ready1"):
        pl.semaphore_wait(ready.at[1], met(2))
    greet(ready.at[2], 4)
    with jax.named_scope("rows_wait"):
        wait(spare.at[1:NX], fr)
    send(fbuf.at[:, c], fbuf.at[:, c], ts, tr, twin)
    with jax.named_scope("across_wait"):
        wait(spare, tr)
    for r in range(NX):
        re = fbuf[r, 0].astype(jnp.float32)[:, :RB]
        im = fbuf[r, 1].astype(jnp.float32)[:, :RB]
        none = jnp.zeros((G, 2 * (RBP - RB)), jnp.float32)
        fstack[r * 2 * G:r * 2 * G + G] = jnp.concatenate([re, -im, none], axis=1).astype(jnp.bfloat16)
        fstack[r * 2 * G + G:(r + 1) * 2 * G] = jnp.concatenate([im, re, none], axis=1).astype(jnp.bfloat16)

    lane = lax.broadcasted_iota(jnp.int32, (16, 128), 1)

    def packed(block):
        tail = block[:, 384:]
        rest = [jnp.where(lane < 96, tail[16 * j:16 * j + 16], pltpu.roll(tail[48:], 96 - 32 * j, 1)) for j in range(3)]
        return jnp.concatenate([block[:, :128], block[:, 128:256], block[:, 256:384], *rest], axis=0)

    def unpacked(block):
        rest = [block[192 + 16 * j:208 + 16 * j] for j in range(3)]
        back = [pltpu.roll(rest[j], 32 * j + 32, 1) for j in range(3)]
        last = jnp.where(lane < 32, back[0], jnp.where(lane < 64, back[1], back[2]))
        tail = jnp.concatenate([*rest, last], axis=0)
        return jnp.concatenate([block[:64], block[64:128], block[128:192], tail], axis=1)

    def produce(p):
        m, w = ORDER[p]
        with jax.named_scope(f"piece_wait{p}"):
            wait(dbuf.at[p, 1:NX], dr.at[p])
        cols = dbuf[p].reshape(NX * 2 * G, 128)
        prod = lax.dot_general(cols, fstack[...], (((0,), (0,)), ((), ())), preferred_element_type=jnp.float32)
        for e in (2 * w + 1, 2 * w):
            block = packed(prod[e % 2 * 64:(e % 2 + 1) * 64])
            if e == 0:
                keep[m] = block
            else:
                csend[m, e] = block.astype(jnp.bfloat16)
                send(csend.at[m, e], crecv.at[m, e], cs, cr.at[m, e], square(e))

    def consume(m):
        block = keep[m]
        for e in (2, 1, 3):
            with jax.named_scope(f"square_wait{m}"):
                wait(crecv.at[m, e], cr.at[m, e])
            block = block + crecv[m, e].astype(jnp.float32)
        if m == 0:
            return block
        if m == 3:
            with jax.named_scope("via_wait"):
                wait(zrecv.at[2], zr.at[2])
            block = block + zrecv[2].astype(jnp.float32)
        zsend[m] = block.astype(jnp.bfloat16)
        send(zsend.at[m], zrecv.at[m], zs, zr.at[m], along(VIA[m]))
        return None

    piece = 0
    greeted = False
    for step in STEPS:
        m = int(step[1])
        if step[0] == "C":
            if not greeted:
                greeted = True
                with jax.named_scope("ready2"):
                    pl.semaphore_wait(ready.at[2], met(4))
            if m == 0:
                acc = consume(m)
            else:
                consume(m)
        else:
            produce(piece)
            piece += 1
    for m in (3, 1):
        with jax.named_scope(f"zwait{m}"):
            wait(zrecv.at[m], zr.at[m])
        acc = acc + zrecv[m].astype(jnp.float32)
    full = unpacked(acc)
    out_ref[:, 0, :] = full[:, :RB]
    out_ref[:, 1, :] = pltpu.roll(full, 2 * RBP - RB, 1)[:, :RB]
    with jax.named_scope("send_waits"):
        wait(s1buf, s1s)
        wait(spare, ts)
        wait(dbuf.at[:, 1:NX], ds)
        wait(csend.at[:, 1:4], cs)
        wait(zsend.at[1:4], zs)


def body(density, coulomb, row_block):
    dma = pltpu.SemaphoreType.DMA
    bf16, f32 = jnp.bfloat16, jnp.float32
    out = pl.pallas_call(
        kernel,
        out_shape=pltpu.VMEM((64, 2, RB), f32),
        in_specs=[pl.BlockSpec(memory_space=pltpu.HBM)] * 3,
        out_specs=pl.BlockSpec(memory_space=pltpu.VMEM),
        scratch_shapes=[
            pltpu.SMEM((1,), jnp.int32),
            pltpu.VMEM((1, G), f32),
            pltpu.VMEM((2, G, COLS), bf16),
            pltpu.VMEM((2, G, RBP), bf16),
            pltpu.VMEM((3, G, RBP), bf16),
            pltpu.VMEM((NX, 2, G, RBP), bf16),
            pltpu.VMEM((NX, G, RBP), bf16),
            pltpu.VMEM((NX * 2 * G, 2 * RBP), bf16),
            pltpu.VMEM((NP, NX, 2 * G, 128), bf16),
            pltpu.VMEM((NP, NX, 2 * G, 128), bf16),
            pltpu.VMEM((4, 4, 240, 128), bf16),
            pltpu.VMEM((4, 4, 240, 128), bf16),
            pltpu.VMEM((4, 240, 128), f32),
            pltpu.VMEM((4, 240, 128), bf16),
            pltpu.VMEM((4, 240, 128), bf16),
            dma((3,)), pltpu.SemaphoreType.REGULAR((3,)), dma, dma, dma, dma, dma, dma,
            dma, dma((NP,)), dma, dma((4, 4)), dma, dma((4,)),
        ],
        compiler_params=pltpu.CompilerParams(collective_id=0, has_side_effects=True),
        name="exchange",
    )(row_block, coulomb.reshape(1, G), density)
    return out.reshape(1, 64, 2, RB)


def solution(mesh):
    return jax.shard_map(
        body,
        mesh=mesh,
        in_specs=(P(None, "ga", "ta"), P("ga"), P()),
        out_specs=P("ta", "ga", None, None),
        check_vma=False,
    )
```

```python
import jax
import jax.numpy as jnp
from jax import lax
from jax.experimental import pallas as pl
from jax.experimental.pallas import tpu as pltpu
from jax.sharding import PartitionSpec as P

MESH = pl.DeviceIdType.MESH
RB = 240
RBP = 256
G = 96
COLS = 4096
WIN = 384
NX, NY, NZ = 4, 2, 8
FAR = (2, 1, 3)
STEPS = ("O2", "W2", "O3", "O1", "W3", "C2", "W1", "C3", "O0", "C1", "W0", "C0")
VIA = {2: 1, 3: 3, 1: 1}
ORDER = tuple((int(step[1]), int(step[0] == "O")) for step in STEPS if step[0] in "OW")
NP = len(ORDER)
EARLY = 2


def place(x, yh, z, yl, c):
    return (yh * (NZ * NX) + z * NX + x, yl * 2 + c)


def kernel(row_hbm, coul_hbm, dens_ref, out_ref, row_ref, coul_ref, dv, wpart, s1buf, fbuf, spare, fstack, sbuf, dbuf, csend, crecv, keep, zsend, zrecv,
           lsem, ready, s1s, s1r, fs, fr, ts, tr, ds, dr, cs, cr, zs, zr):
    ga = lax.axis_index("ga")
    ta = lax.axis_index("ta")
    x, z, yh = ga % NX, (ga // NX) % NZ, ga // (NX * NZ)
    yl, c = ta // 2, ta % 2
    kz, par = z // 2, z % 2

    loads = [pltpu.make_async_copy(a, b, lsem.at[i])
             for i, (a, b) in enumerate(((dens_ref, dv), (row_hbm, row_ref), (coul_hbm, coul_ref)))]
    for load in loads:
        load.start()

    def pair(m):
        a, b = kz // 2, kz % 2
        return (a + m // 2) % 2 * 2 + (b + m % 2) % 2

    def beside(r):
        return place((x + r) % NX, yh, z, yl, c)

    def along(m):
        return place(x, yh, 2 * pair(m) + par, yl, c)

    def square(e):
        return place(x, (yh + e // 2) % NY, 2 * kz + (par + e % 2) % 2, yl, c)

    def mates(q):
        return ((yl + q // 2) % 2, (c + q % 2) % 2)

    twin = place(x, yh, z, yl, (c + 1) % 2)

    bar = pltpu.get_barrier_semaphore()
    peers = [square(2)] + [place(x, yh, z, *mates(q)) for q in range(1, 4)]
    peers += [beside(r) for r in range(1, NX)]
    for peer in peers:
        pl.semaphore_signal(bar, inc=1, device_id=peer, device_id_type=MESH)

    def greet(sem, d):
        @pl.when(z + d < NZ)
        def _():
            pl.semaphore_signal(sem, inc=1, device_id=place(x, yh, z + d, yl, c), device_id_type=MESH)

        @pl.when(z >= d)
        def _():
            pl.semaphore_signal(sem, inc=1, device_id=place(x, yh, z - d, yl, c), device_id_type=MESH)

    def met(d):
        return jnp.where(z + d < NZ, 1, 0) + jnp.where(z >= d, 1, 0)

    greet(bar, 1)

    with jax.named_scope("load_wait"):
        for load in loads:
            load.wait()

    start = row_ref[0] * RB - ta * COLS
    tile = jnp.minimum(jnp.maximum(lax.shift_right_arithmetic(start, 7), 0), (COLS - WIN) // 128)
    src = lax.broadcasted_iota(jnp.int32, (WIN, RBP), 0) + tile * 128
    dst = lax.broadcasted_iota(jnp.int32, (WIN, RBP), 1)
    hit = jnp.logical_and(src == dst + start, dst < RB)
    onehot = jnp.where(hit, 1.0, 0.0).astype(jnp.bfloat16)
    diag = lax.broadcasted_iota(jnp.int32, (G, G), 0) == lax.broadcasted_iota(jnp.int32, (G, G), 1)
    weight = jnp.sum(jnp.where(diag, jnp.broadcast_to(coul_ref[...], (G, G)), 0.0), axis=1, keepdims=True)
    for part in range(2):
        window = dv[part, :, :WIN]
        for k in range(1, (COLS - WIN) // 128 + 1):
            window = jnp.where(tile == k, dv[part, :, k * 128:k * 128 + WIN], window)
        picked = jnp.dot(window, onehot, preferred_element_type=jnp.float32)
        wpart[part] = (weight * picked).astype(jnp.bfloat16)

    low = lax.broadcasted_iota(jnp.int32, (G, 128), 1) < 64

    def pack(p):
        delta, w = ORDER[p]
        y = (yh + w) % NY
        zpair = 2 * pair(delta)
        z0 = zpair + par
        z1 = zpair + (par + 1) % 2
        for part in range(2):
            for h in range(2):
                o0 = pl.multiple_of((y * 16 + z0 * 2 + h) * 128, 128)
                o1 = pl.multiple_of((y * 16 + z1 * 2 + h) * 128, 128)
                t0 = dv[part, :, pl.ds(o0, 128)].astype(jnp.float32)
                t1 = dv[part, :, pl.ds(o1, 128)].astype(jnp.float32)
                even = jnp.where(low, t0, pltpu.roll(t1, 64, 1))
                odd = jnp.where(low, pltpu.roll(t0, 64, 1), t1)
                sbuf[p, 2 * h, part * G:(part + 1) * G, :] = even.astype(jnp.bfloat16)
                sbuf[p, 2 * h + 1, part * G:(part + 1) * G, :] = odd.astype(jnp.bfloat16)
        dbuf[p, 0] = sbuf[p, x]

    def send(src, dst, ss, rs, device):
        pltpu.make_async_remote_copy(src_ref=src, dst_ref=dst, send_sem=ss, recv_sem=rs, device_id=device,
                                     device_id_type=MESH).start()

    def wait(ref, sem):
        pltpu.make_async_copy(ref, ref, sem).wait()

    def spread(p):
        for r in range(1, NX):
            send(sbuf.at[p, (x + r) % NX], dbuf.at[p, r], ds, dr.at[p], beside(r))

    with jax.named_scope("pack0"):
        pack(0)
    with jax.named_scope("bar_wait"):
        pl.semaphore_wait(bar, len(peers) + met(1))

    for q in (2, 3, 1):
        ylq, cq = mates(q)
        send(wpart.at[cq], s1buf.at[q - 1], s1s, s1r, place(x, yh, z, ylq, cq))
    for p in range(EARLY):
        if p > 0:
            pack(p)
        spread(p)
    greet(ready.at[0], 1)
    with jax.named_scope("packs"):
        for p in range(EARLY, NP):
            pack(p)
    with jax.named_scope("ready0"):
        pl.semaphore_wait(ready.at[0], met(1))
    greet(ready.at[1], 2)
    with jax.named_scope("s1_wait"):
        wait(s1buf, s1r)
    total = wpart[c].astype(jnp.float32)
    for q in range(3):
        total = total + s1buf[q].astype(jnp.float32)
    fbuf[0, c] = total.astype(jnp.bfloat16)
    for r in FAR:
        send(fbuf.at[0, c], fbuf.at[r, c], fs, fr, beside(r))
    wait(spare.at[1:NX], fs)
    for p in range(EARLY, NP):
        spread(p)
    with jax.named_scope("ready1"):
        pl.semaphore_wait(ready.at[1], met(2))
    greet(ready.at[2], 4)
    with jax.named_scope("rows_wait"):
        wait(spare.at[1:NX], fr)
    send(fbuf.at[:, c], fbuf.at[:, c], ts, tr, twin)
    with jax.named_scope("across_wait"):
        wait(spare, tr)
    for r in range(NX):
        re = fbuf[r, 0].astype(jnp.float32)[:, :RB]
        im = fbuf[r, 1].astype(jnp.float32)[:, :RB]
        none = jnp.zeros((G, 2 * (RBP - RB)), jnp.float32)
        fstack[r * 2 * G:r * 2 * G + G] = jnp.concatenate([re, -im, none], axis=1).astype(jnp.bfloat16)
        fstack[r * 2 * G + G:(r + 1) * 2 * G] = jnp.concatenate([im, re, none], axis=1).astype(jnp.bfloat16)

    lane = lax.broadcasted_iota(jnp.int32, (16, 128), 1)

    def packed(block):
        tail = block[:, 384:]
        rest = [jnp.where(lane < 96, tail[16 * j:16 * j + 16], pltpu.roll(tail[48:], 96 - 32 * j, 1)) for j in range(3)]
        return jnp.concatenate([block[:, :128], block[:, 128:256], block[:, 256:384], *rest], axis=0)

    def unpacked(block):
        rest = [block[192 + 16 * j:208 + 16 * j] for j in range(3)]
        back = [pltpu.roll(rest[j], 32 * j + 32, 1) for j in range(3)]
        last = jnp.where(lane < 32, back[0], jnp.where(lane < 64, back[1], back[2]))
        tail = jnp.concatenate([*rest, last], axis=0)
        return jnp.concatenate([block[:64], block[64:128], block[128:192], tail], axis=1)

    def produce(p):
        m, w = ORDER[p]
        with jax.named_scope(f"piece_wait{p}"):
            wait(dbuf.at[p, 1:NX], dr.at[p])
        cols = dbuf[p].reshape(NX * 2 * G, 128)
        prod = lax.dot_general(cols, fstack[...], (((0,), (0,)), ((), ())), preferred_element_type=jnp.float32)
        for e in (2 * w + 1, 2 * w):
            block = packed(prod[e % 2 * 64:(e % 2 + 1) * 64])
            if e == 0:
                keep[m] = block
            else:
                csend[m, e] = block.astype(jnp.bfloat16)
                send(csend.at[m, e], crecv.at[m, e], cs, cr.at[m, e], square(e))

    def consume(m):
        block = keep[m]
        for e in (2, 1, 3):
            with jax.named_scope(f"square_wait{m}"):
                wait(crecv.at[m, e], cr.at[m, e])
            block = block + crecv[m, e].astype(jnp.float32)
        if m == 0:
            return block
        if m == 3:
            with jax.named_scope("via_wait"):
                wait(zrecv.at[2], zr.at[2])
            block = block + zrecv[2].astype(jnp.float32)
        zsend[m] = block.astype(jnp.bfloat16)
        send(zsend.at[m], zrecv.at[m], zs, zr.at[m], along(VIA[m]))
        return None

    piece = 0
    greeted = False
    for step in STEPS:
        m = int(step[1])
        if step[0] == "C":
            if not greeted:
                greeted = True
                with jax.named_scope("ready2"):
                    pl.semaphore_wait(ready.at[2], met(4))
            if m == 0:
                acc = consume(m)
            else:
                consume(m)
        else:
            produce(piece)
            piece += 1
    for m in (3, 1):
        with jax.named_scope(f"zwait{m}"):
            wait(zrecv.at[m], zr.at[m])
        acc = acc + zrecv[m].astype(jnp.float32)
    full = unpacked(acc)
    out_ref[:, 0, :] = full[:, :RB]
    out_ref[:, 1, :] = pltpu.roll(full, 2 * RBP - RB, 1)[:, :RB]
    with jax.named_scope("send_waits"):
        wait(s1buf, s1s)
        wait(spare, ts)
        wait(dbuf.at[:, 1:NX], ds)
        wait(csend.at[:, 1:4], cs)
        wait(zsend.at[1:4], zs)


def body(density, coulomb, row_block):
    dma = pltpu.SemaphoreType.DMA
    bf16, f32 = jnp.bfloat16, jnp.float32
    out = pl.pallas_call(
        kernel,
        out_shape=pltpu.VMEM((64, 2, RB), f32),
        in_specs=[pl.BlockSpec(memory_space=pltpu.HBM)] * 3,
        out_specs=pl.BlockSpec(memory_space=pltpu.VMEM),
        scratch_shapes=[
            pltpu.SMEM((1,), jnp.int32),
            pltpu.VMEM((1, G), f32),
            pltpu.VMEM((2, G, COLS), bf16),
            pltpu.VMEM((2, G, RBP), bf16),
            pltpu.VMEM((3, G, RBP), bf16),
            pltpu.VMEM((NX, 2, G, RBP), bf16),
            pltpu.VMEM((NX, G, RBP), bf16),
            pltpu.VMEM((NX * 2 * G, 2 * RBP), bf16),
            pltpu.VMEM((NP, NX, 2 * G, 128), bf16),
            pltpu.VMEM((NP, NX, 2 * G, 128), bf16),
            pltpu.VMEM((4, 4, 240, 128), bf16),
            pltpu.VMEM((4, 4, 240, 128), bf16),
            pltpu.VMEM((4, 240, 128), f32),
            pltpu.VMEM((4, 240, 128), bf16),
            pltpu.VMEM((4, 240, 128), bf16),
            dma((3,)), pltpu.SemaphoreType.REGULAR((3,)), dma, dma, dma, dma, dma, dma,
            dma, dma((NP,)), dma, dma((4, 4)), dma, dma((4,)),
        ],
        compiler_params=pltpu.CompilerParams(collective_id=0, has_side_effects=True),
        name="exchange",
    )(row_block, coulomb.reshape(1, G), density)
    return out.reshape(1, 64, 2, RB)


def solution(mesh):
    return jax.shard_map(
        body,
        mesh=mesh,
        in_specs=(P(None, "ga", "ta"), P("ga"), P()),
        out_specs=P("ta", "ga", None, None),
        check_vma=False,
    )
```

```python
import jax
import jax.numpy as jnp
from jax import lax
from jax.experimental import pallas as pl
from jax.experimental.pallas import tpu as pltpu
from jax.sharding import PartitionSpec as P

MESH = pl.DeviceIdType.MESH
RB = 240
RBP = 256
G = 96
COLS = 4096
WIN = 384
NX, NY, NZ = 4, 2, 8
FAR = (2, 1, 3)
STEPS = ("O2", "W2", "O3", "O1", "W3", "C2", "W1", "C3", "O0", "C1", "W0", "C0")
VIA = {2: 1, 3: 3, 1: 1}
ORDER = tuple((int(step[1]), int(step[0] == "O")) for step in STEPS if step[0] in "OW")
NP = len(ORDER)
EARLY = 2


def place(x, yh, z, yl, c):
    return (yh * (NZ * NX) + z * NX + x, yl * 2 + c)


def kernel(row_hbm, coul_hbm, dens_ref, out_ref, row_ref, coul_ref, dv, wpart, s1buf, fbuf, spare, fstack, sbuf, dbuf, csend, crecv, keep, zsend, zrecv,
           lsem, ready, s1s, s1r, fs, fr, ts, tr, ds, dr, cs, cr, zs, zr):
    ga = lax.axis_index("ga")
    ta = lax.axis_index("ta")
    x, z, yh = ga % NX, (ga // NX) % NZ, ga // (NX * NZ)
    yl, c = ta // 2, ta % 2
    kz, par = z // 2, z % 2

    loads = [pltpu.make_async_copy(a, b, lsem.at[i])
             for i, (a, b) in enumerate(((dens_ref, dv), (row_hbm, row_ref), (coul_hbm, coul_ref)))]
    for load in loads:
        load.start()

    def pair(m):
        a, b = kz // 2, kz % 2
        return (a + m // 2) % 2 * 2 + (b + m % 2) % 2

    def beside(r):
        return place((x + r) % NX, yh, z, yl, c)

    def along(m):
        return place(x, yh, 2 * pair(m) + par, yl, c)

    def square(e):
        return place(x, (yh + e // 2) % NY, 2 * kz + (par + e % 2) % 2, yl, c)

    def mates(q):
        return ((yl + q // 2) % 2, (c + q % 2) % 2)

    twin = place(x, yh, z, yl, (c + 1) % 2)

    bar = pltpu.get_barrier_semaphore()
    peers = [square(2)] + [place(x, yh, z, *mates(q)) for q in range(1, 4)]
    peers += [beside(r) for r in range(1, NX)]
    for peer in peers:
        pl.semaphore_signal(bar, inc=1, device_id=peer, device_id_type=MESH)

    def greet(sem, d):
        @pl.when(z + d < NZ)
        def _():
            pl.semaphore_signal(sem, inc=1, device_id=place(x, yh, z + d, yl, c), device_id_type=MESH)

        @pl.when(z >= d)
        def _():
            pl.semaphore_signal(sem, inc=1, device_id=place(x, yh, z - d, yl, c), device_id_type=MESH)

    def met(d):
        return jnp.where(z + d < NZ, 1, 0) + jnp.where(z >= d, 1, 0)

    greet(bar, 1)

    with jax.named_scope("load_wait"):
        for load in loads:
            load.wait()

    start = row_ref[0] * RB - ta * COLS
    tile = jnp.minimum(jnp.maximum(lax.shift_right_arithmetic(start, 7), 0), (COLS - WIN) // 128)
    src = lax.broadcasted_iota(jnp.int32, (WIN, RBP), 0) + tile * 128
    dst = lax.broadcasted_iota(jnp.int32, (WIN, RBP), 1)
    hit = jnp.logical_and(src == dst + start, dst < RB)
    onehot = jnp.where(hit, 1.0, 0.0).astype(jnp.bfloat16)
    diag = lax.broadcasted_iota(jnp.int32, (G, G), 0) == lax.broadcasted_iota(jnp.int32, (G, G), 1)
    weight = jnp.sum(jnp.where(diag, jnp.broadcast_to(coul_ref[...], (G, G)), 0.0), axis=1, keepdims=True)
    for part in range(2):
        window = dv[part, :, :WIN]
        for k in range(1, (COLS - WIN) // 128 + 1):
            window = jnp.where(tile == k, dv[part, :, k * 128:k * 128 + WIN], window)
        picked = jnp.dot(window, onehot, preferred_element_type=jnp.float32)
        wpart[part] = (weight * picked).astype(jnp.bfloat16)

    low = lax.broadcasted_iota(jnp.int32, (G, 128), 1) < 64

    def pack(p):
        delta, w = ORDER[p]
        y = (yh + w) % NY
        zpair = 2 * pair(delta)
        z0 = zpair + par
        z1 = zpair + (par + 1) % 2
        for part in range(2):
            for h in range(2):
                o0 = pl.multiple_of((y * 16 + z0 * 2 + h) * 128, 128)
                o1 = pl.multiple_of((y * 16 + z1 * 2 + h) * 128, 128)
                t0 = dv[part, :, pl.ds(o0, 128)].astype(jnp.float32)
                t1 = dv[part, :, pl.ds(o1, 128)].astype(jnp.float32)
                even = jnp.where(low, t0, pltpu.roll(t1, 64, 1))
                odd = jnp.where(low, pltpu.roll(t0, 64, 1), t1)
                sbuf[p, 2 * h, part * G:(part + 1) * G, :] = even.astype(jnp.bfloat16)
                sbuf[p, 2 * h + 1, part * G:(part + 1) * G, :] = odd.astype(jnp.bfloat16)
        dbuf[p, 0] = sbuf[p, x]

    def send(src, dst, ss, rs, device):
        pltpu.make_async_remote_copy(src_ref=src, dst_ref=dst, send_sem=ss, recv_sem=rs, device_id=device,
                                     device_id_type=MESH).start()

    def wait(ref, sem):
        pltpu.make_async_copy(ref, ref, sem).wait()

    def spread(p):
        for r in range(1, NX):
            send(sbuf.at[p, (x + r) % NX], dbuf.at[p, r], ds, dr.at[p], beside(r))

    with jax.named_scope("pack0"):
        pack(0)
    with jax.named_scope("bar_wait"):
        pl.semaphore_wait(bar, len(peers) + met(1))

    for q in (2, 3, 1):
        ylq, cq = mates(q)
        send(wpart.at[cq], s1buf.at[q - 1], s1s, s1r, place(x, yh, z, ylq, cq))
    for p in range(EARLY):
        if p > 0:
            pack(p)
        spread(p)
    greet(ready.at[0], 1)
    with jax.named_scope("packs"):
        for p in range(EARLY, NP):
            pack(p)
    with jax.named_scope("s1_wait"):
        wait(s1buf, s1r)
    total = wpart[c].astype(jnp.float32)
    for q in range(3):
        total = total + s1buf[q].astype(jnp.float32)
    fbuf[0, c] = total.astype(jnp.bfloat16)
    for r in FAR:
        send(fbuf.at[0, c], fbuf.at[r, c], fs, fr, beside(r))
    with jax.named_scope("ready0"):
        pl.semaphore_wait(ready.at[0], met(1))
    greet(ready.at[1], 2)
    wait(spare.at[1:NX], fs)
    for p in range(EARLY, NP):
        spread(p)
    with jax.named_scope("ready1"):
        pl.semaphore_wait(ready.at[1], met(2))
    greet(ready.at[2], 4)
    with jax.named_scope("rows_wait"):
        wait(spare.at[1:NX], fr)
    send(fbuf.at[:, c], fbuf.at[:, c], ts, tr, twin)
    with jax.named_scope("across_wait"):
        wait(spare, tr)
    for r in range(NX):
        re = fbuf[r, 0].astype(jnp.float32)[:, :RB]
        im = fbuf[r, 1].astype(jnp.float32)[:, :RB]
        none = jnp.zeros((G, 2 * (RBP - RB)), jnp.float32)
        fstack[r * 2 * G:r * 2 * G + G] = jnp.concatenate([re, -im, none], axis=1).astype(jnp.bfloat16)
        fstack[r * 2 * G + G:(r + 1) * 2 * G] = jnp.concatenate([im, re, none], axis=1).astype(jnp.bfloat16)

    lane = lax.broadcasted_iota(jnp.int32, (16, 128), 1)

    def packed(block):
        tail = block[:, 384:]
        rest = [jnp.where(lane < 96, tail[16 * j:16 * j + 16], pltpu.roll(tail[48:], 96 - 32 * j, 1)) for j in range(3)]
        return jnp.concatenate([block[:, :128], block[:, 128:256], block[:, 256:384], *rest], axis=0)

    def unpacked(block):
        rest = [block[192 + 16 * j:208 + 16 * j] for j in range(3)]
        back = [pltpu.roll(rest[j], 32 * j + 32, 1) for j in range(3)]
        last = jnp.where(lane < 32, back[0], jnp.where(lane < 64, back[1], back[2]))
        tail = jnp.concatenate([*rest, last], axis=0)
        return jnp.concatenate([block[:64], block[64:128], block[128:192], tail], axis=1)

    def produce(p):
        m, w = ORDER[p]
        with jax.named_scope(f"piece_wait{p}"):
            wait(dbuf.at[p, 1:NX], dr.at[p])
        cols = dbuf[p].reshape(NX * 2 * G, 128)
        prod = lax.dot_general(cols, fstack[...], (((0,), (0,)), ((), ())), preferred_element_type=jnp.float32)
        for e in (2 * w + 1, 2 * w):
            block = packed(prod[e % 2 * 64:(e % 2 + 1) * 64])
            if e == 0:
                keep[m] = block
            else:
                csend[m, e] = block.astype(jnp.bfloat16)
                send(csend.at[m, e], crecv.at[m, e], cs, cr.at[m, e], square(e))

    def consume(m):
        block = keep[m]
        for e in (2, 1, 3):
            with jax.named_scope(f"square_wait{m}"):
                wait(crecv.at[m, e], cr.at[m, e])
            block = block + crecv[m, e].astype(jnp.float32)
        if m == 0:
            return block
        if m == 3:
            with jax.named_scope("via_wait"):
                wait(zrecv.at[2], zr.at[2])
            block = block + zrecv[2].astype(jnp.float32)
        zsend[m] = block.astype(jnp.bfloat16)
        send(zsend.at[m], zrecv.at[m], zs, zr.at[m], along(VIA[m]))
        return None

    piece = 0
    greeted = False
    for step in STEPS:
        m = int(step[1])
        if step[0] == "C":
            if not greeted:
                greeted = True
                with jax.named_scope("ready2"):
                    pl.semaphore_wait(ready.at[2], met(4))
            if m == 0:
                acc = consume(m)
            else:
                consume(m)
        else:
            produce(piece)
            piece += 1
    for m in (3, 1):
        with jax.named_scope(f"zwait{m}"):
            wait(zrecv.at[m], zr.at[m])
        acc = acc + zrecv[m].astype(jnp.float32)
    full = unpacked(acc)
    out_ref[:, 0, :] = full[:, :RB]
    out_ref[:, 1, :] = pltpu.roll(full, 2 * RBP - RB, 1)[:, :RB]
    with jax.named_scope("send_waits"):
        wait(s1buf, s1s)
        wait(spare, ts)
        wait(dbuf.at[:, 1:NX], ds)
        wait(csend.at[:, 1:4], cs)
        wait(zsend.at[1:4], zs)


def body(density, coulomb, row_block):
    dma = pltpu.SemaphoreType.DMA
    bf16, f32 = jnp.bfloat16, jnp.float32
    out = pl.pallas_call(
        kernel,
        out_shape=pltpu.VMEM((64, 2, RB), f32),
        in_specs=[pl.BlockSpec(memory_space=pltpu.HBM)] * 3,
        out_specs=pl.BlockSpec(memory_space=pltpu.VMEM),
        scratch_shapes=[
            pltpu.SMEM((1,), jnp.int32),
            pltpu.VMEM((1, G), f32),
            pltpu.VMEM((2, G, COLS), bf16),
            pltpu.VMEM((2, G, RBP), bf16),
            pltpu.VMEM((3, G, RBP), bf16),
            pltpu.VMEM((NX, 2, G, RBP), bf16),
            pltpu.VMEM((NX, G, RBP), bf16),
            pltpu.VMEM((NX * 2 * G, 2 * RBP), bf16),
            pltpu.VMEM((NP, NX, 2 * G, 128), bf16),
            pltpu.VMEM((NP, NX, 2 * G, 128), bf16),
            pltpu.VMEM((4, 4, 240, 128), bf16),
            pltpu.VMEM((4, 4, 240, 128), bf16),
            pltpu.VMEM((4, 240, 128), f32),
            pltpu.VMEM((4, 240, 128), bf16),
            pltpu.VMEM((4, 240, 128), bf16),
            dma((3,)), pltpu.SemaphoreType.REGULAR((3,)), dma, dma, dma, dma, dma, dma,
            dma, dma((NP,)), dma, dma((4, 4)), dma, dma((4,)),
        ],
        compiler_params=pltpu.CompilerParams(collective_id=0, has_side_effects=True),
        name="exchange",
    )(row_block, coulomb.reshape(1, G), density)
    return out.reshape(1, 64, 2, RB)


def solution(mesh):
    return jax.shard_map(
        body,
        mesh=mesh,
        in_specs=(P(None, "ga", "ta"), P("ga"), P()),
        out_specs=P("ta", "ga", None, None),
        check_vma=False,
    )
```
